8 devices in a mesh: emb: 8 (over z, y, x, core).
Axes of the slice: x: 2, y: 2, z: 1, core: 2. Of those that a mesh axis runs over, the one named last changes fastest.
Arguments:
- uniq_ids: int32 [16384], P('emb')
- inv_map: int32 [32768], P('emb')
- x_in: bfloat16 [32768, 768], P('emb')
- d_out: bfloat16 [32768, 768], P('emb')
- tables: bfloat16 [5, 50304, 768], P(None, 'emb')
- w_up: bfloat16 [5, 768, 3072], replicated
- w_down: bfloat16 [5, 3072, 768], replicated
- w_gate: bfloat16 [5, 768, 768], replicated
- w_proj: bfloat16 [5, 768, 768], replicated
Outputs:
- output 1: bfloat16 [32768, 768], P('emb')
- output 2: float32 [5, 50304, 768], P(None, 'emb')
All inputs are finite; a program needn't handle non-finite values.
Results may differ from the reference program's by a relative error of at most 0.015214.
Values are sent between devices in bfloat16 or wider.
A program may use at most 1 GiB of HBM per device.

```python
import jax
import jax.numpy as jnp
from jax import lax

D_MODEL = 768
D_FF = 3072
D_EMB = 768
VOCAB_SIZE = 50304
LAYERS = 5
N_LOC = 4096
N_UNIQ = 2048
GROUP_SIZE = 8

SHARD_ROWS = VOCAB_SIZE // GROUP_SIZE
CAPACITY = 2 * N_UNIQ // GROUP_SIZE
HOT_OWNERS = GROUP_SIZE // 8
HOT_SLOTS = CAPACITY * HOT_OWNERS
COLD_OWNERS = GROUP_SIZE - HOT_OWNERS
TOKENS = GROUP_SIZE * N_LOC
EPSILON = 1e-6


def shuffle_tokens(perm_key):
    return jax.random.permutation(perm_key, N_LOC)


def draw_routing(route_key):
    split_keys = jax.random.split(route_key, 7)
    hot_base = jax.random.randint(split_keys[0], (HOT_OWNERS,), 0, SHARD_ROWS)
    cold_base = jax.random.randint(split_keys[1], (GROUP_SIZE,), 0, SHARD_ROWS)
    dev_rot = jax.random.randint(split_keys[2], (GROUP_SIZE, 1), 0, COLD_OWNERS)
    dev_mult = jax.random.randint(split_keys[3], (GROUP_SIZE, 1), 0, SHARD_ROWS)
    slot_idx = jnp.arange(N_UNIQ)
    hot_owner = jnp.minimum(slot_idx // CAPACITY, HOT_OWNERS - 1)
    hot_ids = hot_owner * SHARD_ROWS + (hot_base[hot_owner] + slot_idx % CAPACITY) % SHARD_ROWS
    cold_pos = jnp.maximum(slot_idx - HOT_SLOTS, 0)[None, :] + dev_rot
    cold_owner = HOT_OWNERS + cold_pos % COLD_OWNERS
    cold_row = (dev_mult * (cold_owner + 1) + cold_base[cold_owner] + cold_pos // COLD_OWNERS) % SHARD_ROWS
    uniq_ids = jnp.where(slot_idx[None, :] < HOT_SLOTS, hot_ids[None, :], cold_owner * SHARD_ROWS + cold_row)
    live_count = jax.random.randint(split_keys[4], (GROUP_SIZE, 1), N_UNIQ // 2, N_UNIQ + 1)
    live_count = jnp.where(jnp.arange(GROUP_SIZE)[:, None] == 0, N_UNIQ, live_count)
    raw_draws = jax.random.randint(split_keys[5], (3, GROUP_SIZE, N_LOC), 0, 1 << 20) % live_count
    zipf_slot = ((raw_draws[0] * raw_draws[1]) // live_count * raw_draws[2]) // live_count
    tok_idx = jnp.arange(N_LOC)[None, :]
    slot_of_tok = jnp.where(tok_idx < live_count, tok_idx, zipf_slot)
    orders = jax.vmap(shuffle_tokens)(jax.random.split(split_keys[6], GROUP_SIZE))
    inv_map = jnp.take_along_axis(slot_of_tok, orders, axis=1)
    return uniq_ids.reshape(-1).astype(jnp.int32), inv_map.reshape(-1).astype(jnp.int32)


def setup_inputs(seed: int = 0) -> dict:
    base_key = jax.random.key(seed)
    sub_keys = jax.random.split(base_key, 8)
    uniq_ids, inv_map = draw_routing(sub_keys[0])
    x_in = jax.random.normal(sub_keys[1], (TOKENS, D_MODEL), jnp.float32).astype(jnp.bfloat16)
    d_out = jax.random.normal(sub_keys[2], (TOKENS, D_MODEL), jnp.float32).astype(jnp.bfloat16)
    tables = (0.4 * jax.random.normal(sub_keys[3], (LAYERS, VOCAB_SIZE, D_EMB), jnp.float32)).astype(jnp.bfloat16)
    w_up = (jax.random.normal(sub_keys[4], (LAYERS, D_MODEL, D_FF), jnp.float32) * D_MODEL ** -0.5).astype(jnp.bfloat16)
    w_down = (jax.random.normal(sub_keys[5], (LAYERS, D_FF, D_MODEL), jnp.float32) * (0.5 * D_FF ** -0.5)).astype(jnp.bfloat16)
    w_gate = (jax.random.normal(sub_keys[6], (LAYERS, D_MODEL, D_EMB), jnp.float32) * D_MODEL ** -0.5).astype(jnp.bfloat16)
    w_proj = (jax.random.normal(sub_keys[7], (LAYERS, D_EMB, D_MODEL), jnp.float32) * D_EMB ** -0.5).astype(jnp.bfloat16)
    return {'uniq_ids': uniq_ids, 'inv_map': inv_map, 'x_in': x_in, 'd_out': d_out, 'tables': tables,
            'w_up': w_up, 'w_down': w_down, 'w_gate': w_gate, 'w_proj': w_proj}


def gelu_tanh(pre_act):
    return jax.nn.gelu(pre_act, approximate=True)


def norm_rows(x):
    x_f = x.astype(jnp.float32)
    inv_rms = lax.rsqrt(jnp.mean(x_f * x_f, axis=-1, keepdims=True) + EPSILON)
    return x_f * inv_rms, inv_rms


def layer_forward(x, tok_rows, w_up, w_down, w_gate, w_proj):
    normed = norm_rows(x)[0]
    u_bf = normed.astype(jnp.bfloat16)
    hidden = gelu_tanh(jnp.dot(u_bf, w_up, preferred_element_type=jnp.float32)).astype(jnp.bfloat16)
    mlp_out = jnp.dot(hidden, w_down, preferred_element_type=jnp.float32).astype(jnp.bfloat16)
    gate_act = gelu_tanh(jnp.dot(u_bf, w_gate, preferred_element_type=jnp.float32)).astype(jnp.bfloat16)
    mixed = (gate_act.astype(jnp.float32) * tok_rows.astype(jnp.float32)).astype(jnp.bfloat16)
    proj_out = jnp.dot(mixed, w_proj, preferred_element_type=jnp.float32).astype(jnp.bfloat16)
    return (x.astype(jnp.float32) + mlp_out.astype(jnp.float32) + proj_out.astype(jnp.float32)).astype(jnp.bfloat16)


def layer_backward(x, tok_rows, cotangent, w_up, w_down, w_gate, w_proj):
    normed, inv_rms = norm_rows(x)
    u_bf = normed.astype(jnp.bfloat16)
    pre_up = jnp.dot(u_bf, w_up, preferred_element_type=jnp.float32)
    pre_gate = jnp.dot(u_bf, w_gate, preferred_element_type=jnp.float32)
    gate_act = gelu_tanh(pre_gate).astype(jnp.bfloat16)
    d_mixed = jnp.dot(cotangent, w_proj.T, preferred_element_type=jnp.float32).astype(jnp.bfloat16)
    row_grad = gate_act.astype(jnp.float32) * d_mixed.astype(jnp.float32)
    d_hidden = jnp.dot(cotangent, w_down.T, preferred_element_type=jnp.float32).astype(jnp.bfloat16)
    d_pre_up = jax.vjp(gelu_tanh, pre_up)[1](d_hidden.astype(jnp.float32))[0].astype(jnp.bfloat16)
    d_pre_gate = jax.vjp(gelu_tanh, pre_gate)[1](d_mixed.astype(jnp.float32) * tok_rows.astype(jnp.float32))[0].astype(jnp.bfloat16)
    d_normed = (jnp.dot(d_pre_up, w_up.T, preferred_element_type=jnp.float32)
                + jnp.dot(d_pre_gate, w_gate.T, preferred_element_type=jnp.float32))
    d_x = inv_rms * (d_normed - normed * jnp.mean(d_normed * normed, axis=-1, keepdims=True))
    return (cotangent.astype(jnp.float32) + d_x).astype(jnp.bfloat16), row_grad


def reference(uniq_ids, inv_map, x_in, d_out, tables, w_up, w_down, w_gate, w_proj):
    tok_dev = jnp.arange(TOKENS) // N_LOC
    tok_ids = uniq_ids[tok_dev * N_UNIQ + inv_map]

    def fwd_step(x, layer_args):
        table_l, up_l, down_l, gate_l, proj_l = layer_args
        return layer_forward(x, table_l[tok_ids], up_l, down_l, gate_l, proj_l), x

    x_out, x_saved = lax.scan(fwd_step, x_in, (tables, w_up, w_down, w_gate, w_proj))

    def bwd_step(cotangent, layer_args):
        x_l, table_l, up_l, down_l, gate_l, proj_l = layer_args
        new_cot, row_grad = layer_backward(x_l, table_l[tok_ids], cotangent, up_l, down_l, gate_l, proj_l)
        return new_cot, jax.ops.segment_sum(row_grad, tok_ids, num_segments=VOCAB_SIZE)

    d_tables = lax.scan(bwd_step, d_out, (x_saved, tables, w_up, w_down, w_gate, w_proj), reverse=True)[1]
    return x_out, d_tables
```

```python
import functools

import jax
import jax.numpy as jnp
from jax import lax
from jax.experimental import pallas as pl
from jax.experimental.pallas import tpu as pltpu
from jax.sharding import PartitionSpec as P

EPSILON = 1e-6
BF16 = jnp.bfloat16
F32 = jnp.float32
I32 = jnp.int32

CH = 16
SUB = 256
WIN = 384
TB = 512
FC = 512
VMEM_LIMIT = 60 * 1024 * 1024
G0 = 0.7978845608028654
G1 = G0 * 0.044715


def dot(a, b):
    return jnp.dot(a, b, preferred_element_type=F32)


def dot_nt(a, b):
    return lax.dot_general(a, b, (((1,), (1,)), ((), ())), preferred_element_type=F32)


def gelu(a):
    half = 0.5 * a
    return half * jnp.tanh(a * (G0 + G1 * (a * a))) + half


def gelu_grad(a):
    sq = a * a
    t = jnp.tanh(a * (G0 + G1 * sq))
    return 0.5 * t + 0.5 + (0.5 * a * (1.0 - t * t)) * (G0 + (3.0 * G1) * sq)


def norm_rows(xf):
    inv = lax.rsqrt(jnp.mean(xf * xf, axis=-1, keepdims=True) + EPSILON)
    return xf * inv, inv


def fwd_kernel(wst, chunk, x_ref, posc_ref, up_ref, dn_ref, gt_ref, pj_ref, ret_ref,
               xo_ref, e_ref, rows, sem):
    i = pl.program_id(0)
    n_rows = rows.shape[0]

    @pl.when(i == 0)
    def _():
        def start(d, carry):
            src = pl.multiple_of(chunk[d] * CH, CH)
            dst = pl.multiple_of(d * CH, CH)
            pltpu.make_async_copy(ret_ref.at[pl.ds(src, CH)], rows.at[pl.ds(dst, CH)], sem).start()
            return carry

        lax.fori_loop(0, n_rows // CH, start, 0)
        pltpu.make_async_copy(ret_ref.at[pl.ds(0, n_rows)], rows, sem).wait()

    tb = x_ref.shape[0]
    xf = x_ref[...].astype(F32)
    u = norm_rows(xf)[0].astype(BF16)
    parts = []
    for q in range(tb // SUB):
        w0 = pl.multiple_of(wst[i * (tb // SUB) + q] * CH, CH)
        col = posc_ref[q * SUB:(q + 1) * SUB, :] - w0
        hot = jnp.where(col == lax.broadcasted_iota(I32, (SUB, WIN), 1), 1.0, 0.0).astype(BF16)
        parts.append(dot(hot, rows[pl.ds(w0, WIN), :]).astype(BF16))
    e = jnp.concatenate(parts, axis=0)
    e_ref[...] = e
    g = gelu(dot(u, gt_ref[0])).astype(BF16)
    z = (g.astype(F32) * e.astype(F32)).astype(BF16)
    proj = dot(z, pj_ref[0]).astype(BF16)
    ff = up_ref.shape[2]
    mlp = None
    for k in range(ff // FC):
        h = gelu(dot(u, up_ref[0, :, k * FC:(k + 1) * FC])).astype(BF16)
        part = dot(h, dn_ref[0, k * FC:(k + 1) * FC, :])
        mlp = part if mlp is None else mlp + part
    xo_ref[...] = (xf + mlp.astype(BF16).astype(F32) + proj.astype(F32)).astype(BF16)


def rowgrad_kernel(wst, chunk, total, x_ref, c_ref, posr_ref, gt_ref, pj_ref,
                   s_ref, send_ref, acc, sem):
    i = pl.program_id(0)
    last = pl.num_programs(0) - 1

    @pl.when(i == 0)
    def _():
        acc[...] = jnp.zeros_like(acc)

    tb = x_ref.shape[0]
    u = norm_rows(x_ref[...].astype(F32))[0].astype(BF16)
    g = gelu(dot(u, gt_ref[0])).astype(BF16)
    s = dot_nt(c_ref[...], pj_ref[0]).astype(BF16)
    s_ref[...] = s
    k = g.astype(F32) * s.astype(F32)
    hi = k.astype(BF16)
    lo = (k - hi.astype(F32)).astype(BF16)
    for q in range(tb // SUB):
        w0 = pl.multiple_of(wst[i * (tb // SUB) + q] * CH, CH)
        row = posr_ref[q] - w0
        hot = jnp.where(row == lax.broadcasted_iota(I32, (WIN, SUB), 0), 1.0, 0.0).astype(BF16)
        sl = slice(q * SUB, (q + 1) * SUB)
        acc[pl.ds(w0, WIN), :] += dot(hot, hi[sl]) + dot(hot, lo[sl])

    @pl.when(i == last)
    def _():
        def copy(d):
            dst = pl.multiple_of(chunk[d] * CH, CH)
            src = pl.multiple_of(d * CH, CH)
            return pltpu.make_async_copy(acc.at[pl.ds(src, CH)], send_ref.at[pl.ds(dst, CH)], sem)

        def start(d, carry):
            copy(d).start()
            return carry

        def wait(d, carry):
            copy(d).wait()
            return carry

        lax.fori_loop(0, total[0], start, 0)
        lax.fori_loop(0, total[0], wait, 0)


def bwd_kernel(x_ref, c_ref, s_ref, e_ref, up_ref, dn_ref, gt_ref, co_ref):
    xf = x_ref[...].astype(F32)
    n, inv = norm_rows(xf)
    u = n.astype(BF16)
    c = c_ref[...]
    b = dot(u, gt_ref[0])
    db = (gelu_grad(b) * (s_ref[...].astype(F32) * e_ref[...].astype(F32))).astype(BF16)
    du = dot_nt(db, gt_ref[0])
    ff = up_ref.shape[2]
    for k in range(ff // FC):
        w_k = up_ref[0, :, k * FC:(k + 1) * FC]
        a = dot(u, w_k)
        dh = dot_nt(c, dn_ref[0, k * FC:(k + 1) * FC, :]).astype(BF16)
        da = (gelu_grad(a) * dh.astype(F32)).astype(BF16)
        du = du + dot_nt(da, w_k)
    dx = inv * (du - n * jnp.mean(du * n, axis=-1, keepdims=True))
    co_ref[...] = (c.astype(F32) + dx).astype(BF16)


def scatter_body(layer, row_of, count, recv_ref, out_ref, acc, sem):
    i = pl.program_id(0)
    cap = recv_ref.shape[0]

    @pl.when(i == 0)
    def _():
        acc[...] = jnp.zeros_like(acc)

    def group(t, carry):
        base = pl.multiple_of(t * 8, 8)
        idx = [row_of[i * cap + base + q] for q in range(8)]
        old = [acc[pl.ds(r, 1), :] for r in idx]
        new = [o + recv_ref[pl.ds(base + q, 1), :] for q, o in enumerate(old)]
        for r, v in zip(idx, new):
            acc[pl.ds(r, 1), :] = v
        return carry

    lax.fori_loop(0, (count[i] + 7) // 8, group, 0)

    @pl.when(i == pl.num_programs(0) - 1)
    def _():
        cp = pltpu.make_async_copy(acc.at[pl.ds(0, out_ref.shape[1])], out_ref.at[layer], sem)
        cp.start()
        cp.wait()


def scatter_first(layer, row_of, count, recv_ref, out_ref, acc, sem):
    scatter_body(layer, row_of, count, recv_ref, out_ref, acc, sem)


def scatter_next(layer, row_of, count, recv_ref, _, out_ref, acc, sem):
    scatter_body(layer, row_of, count, recv_ref, out_ref, acc, sem)


ANY = pl.BlockSpec(memory_space=pl.ANY)


def once(shape, index_map):
    return pl.BlockSpec(shape, index_map, pipeline_mode=pl.Buffered(1))


def params():
    return pltpu.CompilerParams(dimension_semantics=("arbitrary",), vmem_limit_bytes=VMEM_LIMIT)


def cost(flops, nbytes):
    return pl.CostEstimate(flops=int(flops), bytes_accessed=int(nbytes), transcendentals=0)


def solution(mesh):
    group_size = mesh.shape['emb']

    def body(uniq_loc, inv_loc, x_loc, dy_loc, tab_loc, w_up, w_down, w_gate, w_proj):
        layers, shard_rows, d_emb = tab_loc.shape
        n_uniq = uniq_loc.shape[0]
        n_tok, d_model = x_loc.shape
        ff = w_up.shape[2]
        capacity = 2 * n_uniq // group_size
        slots = group_size * capacity
        cap_ch = capacity // CH
        row_chunks = (n_uniq + group_size * CH + WIN) // CH
        n_rows = row_chunks * CH
        my_dev = lax.axis_index('emb')

        iota = jnp.arange(n_tok, dtype=I32)
        tok_id = uniq_loc.at[inv_loc].get(mode='promise_in_bounds')
        order = lax.sort(tok_id * n_tok + iota)
        perm = order % n_tok
        sid = order // n_tok
        unperm = lax.sort(perm * n_tok + iota) % n_tok
        is_new = jnp.concatenate([jnp.ones((1,), jnp.bool_), sid[1:] != sid[:-1]])
        rank = jnp.cumsum(is_new.astype(I32)) - 1
        used = lax.sort(jnp.where(is_new, sid, jnp.int32(2 ** 30)))[:n_uniq]
        owners = jnp.arange(group_size, dtype=I32)
        own = sid // shard_rows
        own_hot = own[None, :] == owners[:, None]
        cnt = jnp.sum(jnp.where(own_hot & is_new[None, :], 1, 0), axis=1).astype(I32)
        first = (jnp.cumsum(cnt) - cnt).astype(I32)
        n_ch = (cnt + CH - 1) // CH
        first_ch = (jnp.cumsum(n_ch) - n_ch).astype(I32)
        pos = rank + jnp.sum(jnp.where(own_hot, (first_ch * CH - first)[:, None], 0), axis=0)
        pos = pos.astype(I32)
        wst = pos.reshape(n_tok // SUB, SUB)[:, 0] // CH
        cid = jnp.arange(row_chunks, dtype=I32)[None, :]
        in_own = (cid >= first_ch[:, None]) & (cid < (first_ch + n_ch)[:, None])
        chunk = jnp.sum(jnp.where(in_own, owners[:, None] * cap_ch + cid - first_ch[:, None], 0), axis=0).astype(I32)
        total = jnp.sum(n_ch).astype(I32).reshape(1)
        used_pad = jnp.concatenate([used, jnp.full((capacity,), -1, I32)])
        kk = jnp.arange(capacity, dtype=I32)
        send_ids = jnp.stack([
            jnp.where(kk < cnt[j], lax.dynamic_slice(used_pad, (first[j],), (capacity,)), -1)
            for j in range(group_size)])
        recv_ids = lax.all_to_all(send_ids, 'emb', 0, 0)
        valid = recv_ids >= 0
        local_row = recv_ids - my_dev * shard_rows
        fetch_row = jnp.where(valid, local_row, 0).reshape(-1)
        add_row = jnp.where(valid, local_row, shard_rows).reshape(-1)
        add_cnt = jnp.sum(valid.astype(I32), axis=1).astype(I32)
        posc = pos.reshape(n_tok, 1)
        posr = pos.reshape(n_tok // SUB, 1, SUB)
        flat_tab = tab_loc.reshape(layers * shard_rows, d_emb)

        tok_spec = pl.BlockSpec((TB, d_model), lambda i, *_: (i, 0))
        posr_spec = pl.BlockSpec((TB // SUB, 1, SUB), lambda i, *_: (i, 0, 0))
        grid = (n_tok // TB,)
        tok_out = jax.ShapeDtypeStruct((n_tok, d_model), BF16)

        def w_specs(layer, *shapes):
            return [once((1,) + s, lambda i, *_, layer=layer: (layer, 0, 0)) for s in shapes]

        s_up, s_dn, s_sq = (d_model, ff), (ff, d_model), (d_model, d_emb)
        mm = 2.0 * n_tok * d_model * ff
        sq = 2.0 * n_tok * d_model * d_emb

        def forward(layer, x, returned):
            return pl.pallas_call(
                fwd_kernel, out_shape=[tok_out, tok_out],
                grid_spec=pltpu.PrefetchScalarGridSpec(
                    num_scalar_prefetch=2, grid=grid,
                    in_specs=[tok_spec, pl.BlockSpec((TB, 1), lambda i, *_: (i, 0)),
                              *w_specs(layer, s_up, s_dn, s_sq, s_sq), ANY],
                    out_specs=[tok_spec, tok_spec],
                    scratch_shapes=[pltpu.VMEM((n_rows, d_emb), BF16), pltpu.SemaphoreType.DMA]),
                compiler_params=params(), name='fwd',
                cost_estimate=cost(2 * mm + 2 * sq, 3e7),
            )(wst, chunk, x, posc, w_up, w_down, w_gate, w_proj, returned)

        def rowgrad(layer, x, c):
            return pl.pallas_call(
                rowgrad_kernel, out_shape=[tok_out, jax.ShapeDtypeStruct((slots, d_emb), F32)],
                grid_spec=pltpu.PrefetchScalarGridSpec(
                    num_scalar_prefetch=3, grid=grid,
                    in_specs=[tok_spec, tok_spec, posr_spec, *w_specs(layer, s_sq, s_sq)],
                    out_specs=[tok_spec, ANY],
                    scratch_shapes=[pltpu.VMEM((n_rows, d_emb), F32), pltpu.SemaphoreType.DMA]),
                compiler_params=params(), name='rowgrad',
                cost_estimate=cost(2 * sq, 3e7),
            )(wst, chunk, total, x, c, posr, w_gate, w_proj)

        def backward(layer, x, c, s, e):
            return pl.pallas_call(
                bwd_kernel, out_shape=tok_out, grid=grid,
                in_specs=[tok_spec] * 4 + w_specs(layer, s_up, s_dn, s_sq),
                out_specs=tok_spec,
                compiler_params=params(), name='bwd',
                cost_estimate=cost(3 * mm + 2 * sq, 4e7),
            )(x, c, s, e, w_up, w_down, w_gate)

        def scatter(layer, received, grads):
            ins = [pl.BlockSpec((capacity, d_emb), lambda i, *_: (i, 0))]
            args = [received]
            if grads is not None:
                ins.append(ANY)
                args.append(grads)
            return pl.pallas_call(
                functools.partial(scatter_first if grads is None else scatter_next, layer),
                out_shape=jax.ShapeDtypeStruct((layers, shard_rows, d_emb), F32),
                grid_spec=pltpu.PrefetchScalarGridSpec(
                    num_scalar_prefetch=2, grid=(group_size,), in_specs=ins, out_specs=ANY,
                    scratch_shapes=[pltpu.VMEM((shard_rows + 8, d_emb), F32), pltpu.SemaphoreType.DMA]),
                compiler_params=params(), name='scatter',
                input_output_aliases={} if grads is None else {3: 0},
                cost_estimate=cost(1e10, 4e7),
            )(add_row, add_cnt, *args)

        def serve(layer, index):
            rows = flat_tab.at[index + layer * shard_rows].get(mode='promise_in_bounds')
            return rows.reshape(group_size, capacity, d_emb)

        def exchange(a):
            return lax.all_to_all(a, 'emb', 0, 0)

        served = serve(0, fetch_row)
        got = exchange(served)
        perm, served, later = lax.optimization_barrier((perm, served, fetch_row))
        x = x_loc.at[perm].get(mode='promise_in_bounds')
        c = dy_loc.at[perm].get(mode='promise_in_bounds')
        served = serve(1, later)
        saved_x, saved_e = [], []
        for layer in range(layers):
            here = got
            if layer + 1 < layers:
                x, c, here, served, later = lax.optimization_barrier((x, c, here, served, later))
                got = exchange(served)
                if layer + 2 < layers:
                    served = serve(layer + 2, later)
            saved_x.append(x)
            x, e = forward(layer, x, here.reshape(slots, d_emb))
            saved_e.append(e)
        x_out = x.at[unperm].get(mode='promise_in_bounds')

        grads = None
        pending = None
        for layer in reversed(range(layers)):
            s, send = rowgrad(layer, saved_x[layer], c)
            got = lax.all_to_all(send.reshape(group_size, capacity, d_emb), 'emb', 0, 0).reshape(slots, d_emb)
            if pending is not None:
                c, pending = lax.optimization_barrier((c, pending))
                grads = scatter(layer + 1, pending, grads)
            if layer > 0:
                c = backward(layer, saved_x[layer], c, s, saved_e[layer])
            pending = got
        grads = scatter(0, pending, grads)
        return x_out, grads

    return jax.shard_map(body, mesh=mesh,
                         in_specs=(P('emb'), P('emb'), P('emb', None), P('emb', None), P(None, 'emb', None),
                                   P(), P(), P(), P()),
                         out_specs=(P('emb', None), P(None, 'emb', None)), check_vma=False)
```

```python
import functools

import jax
import jax.numpy as jnp
from jax import lax
from jax.experimental import pallas as pl
from jax.experimental.pallas import tpu as pltpu
from jax.sharding import PartitionSpec as P

EPSILON = 1e-6
BF16 = jnp.bfloat16
F32 = jnp.float32
I32 = jnp.int32

CH = 16
SUB = 256
WIN = 384
TB = 512
PIECES = 6
PAD = 16
FC = 512
VMEM_LIMIT = 60 * 1024 * 1024
G0 = 0.7978845608028654
G1 = G0 * 0.044715


def dot(a, b):
    return jnp.dot(a, b, preferred_element_type=F32)


def dot_nt(a, b):
    return lax.dot_general(a, b, (((1,), (1,)), ((), ())), preferred_element_type=F32)


def gelu(a):
    half = 0.5 * a
    return half * jnp.tanh(a * (G0 + G1 * (a * a))) + half


def gelu_grad(a):
    sq = a * a
    t = jnp.tanh(a * (G0 + G1 * sq))
    return 0.5 * t + 0.5 + (0.5 * a * (1.0 - t * t)) * (G0 + (3.0 * G1) * sq)


def norm_rows(xf):
    inv = lax.rsqrt(jnp.mean(xf * xf, axis=-1, keepdims=True) + EPSILON)
    return xf * inv, inv


def fwd_kernel(wst, chunk, x_ref, posc_ref, up_ref, dn_ref, gt_ref, pj_ref, ret_ref,
               xo_ref, e_ref, g_ref, rows, sem):
    i = pl.program_id(0)
    n_rows = rows.shape[0]

    @pl.when(i == 0)
    def _():
        def start(d, carry):
            src = pl.multiple_of(chunk[d] * CH, CH)
            dst = pl.multiple_of(d * CH, CH)
            pltpu.make_async_copy(ret_ref.at[pl.ds(src, CH)], rows.at[pl.ds(dst, CH)], sem).start()
            return carry

        lax.fori_loop(0, n_rows // CH, start, 0)
        pltpu.make_async_copy(ret_ref.at[pl.ds(0, n_rows)], rows, sem).wait()

    tb = x_ref.shape[0]
    xf = x_ref[...].astype(F32)
    u = norm_rows(xf)[0].astype(BF16)
    parts = []
    for q in range(tb // SUB):
        w0 = pl.multiple_of(wst[i * (tb // SUB) + q] * CH, CH)
        col = posc_ref[q * SUB:(q + 1) * SUB, :] - w0
        hot = jnp.where(col == lax.broadcasted_iota(I32, (SUB, WIN), 1), 1.0, 0.0).astype(BF16)
        parts.append(dot(hot, rows[pl.ds(w0, WIN), :]).astype(BF16))
    e = jnp.concatenate(parts, axis=0)
    e_ref[...] = e
    g = gelu(dot(u, gt_ref[0])).astype(BF16)
    g_ref[...] = g
    z = (g.astype(F32) * e.astype(F32)).astype(BF16)
    proj = dot(z, pj_ref[0]).astype(BF16)
    ff = up_ref.shape[2]
    mlp = None
    for k in range(ff // FC):
        h = gelu(dot(u, up_ref[0, :, k * FC:(k + 1) * FC])).astype(BF16)
        part = dot(h, dn_ref[0, k * FC:(k + 1) * FC, :])
        mlp = part if mlp is None else mlp + part
    xo_ref[...] = (xf + mlp.astype(BF16).astype(F32) + proj.astype(F32)).astype(BF16)


def rowgrad_top_kernel(wst, chunk, total, x_ref, c_ref, posr_ref, gt_ref, pj_ref, *refs):
    u = norm_rows(x_ref[...].astype(F32))[0].astype(BF16)
    g = gelu(dot(u, gt_ref[0])).astype(BF16)
    rowgrad_body(wst, chunk, total, g, c_ref, posr_ref, pj_ref, *refs)


def rowgrad_kernel(wst, chunk, total, g_ref, c_ref, posr_ref, pj_ref, *refs):
    rowgrad_body(wst, chunk, total, g_ref[...], c_ref, posr_ref, pj_ref, *refs)


def rowgrad_body(wst, chunk, total, g, c_ref, posr_ref, pj_ref, s_ref, send_ref, acc, sem):
    i = pl.program_id(0)
    last = pl.num_programs(0) - 1

    @pl.when(i == 0)
    def _():
        acc[...] = jnp.zeros_like(acc)

    tb = c_ref.shape[0]
    s = dot_nt(c_ref[...], pj_ref[0]).astype(BF16)
    s_ref[...] = s
    k = g.astype(F32) * s.astype(F32)
    hi = k.astype(BF16)
    lo = (k - hi.astype(F32)).astype(BF16)
    for q in range(tb // SUB):
        w0 = pl.multiple_of(wst[i * (tb // SUB) + q] * CH, CH)
        row = posr_ref[q] - w0
        hot = jnp.where(row == lax.broadcasted_iota(I32, (WIN, SUB), 0), 1.0, 0.0).astype(BF16)
        sl = slice(q * SUB, (q + 1) * SUB)
        acc[pl.ds(w0, WIN), :] += dot(hot, hi[sl]) + dot(hot, lo[sl])

    @pl.when(i == last)
    def _():
        def copy(d):
            dst = pl.multiple_of(chunk[d] * CH, CH)
            src = pl.multiple_of(d * CH, CH)
            return pltpu.make_async_copy(acc.at[pl.ds(src, CH)], send_ref.at[pl.ds(dst, CH)], sem)

        def start(d, carry):
            copy(d).start()
            return carry

        def wait(d, carry):
            copy(d).wait()
            return carry

        lax.fori_loop(0, total[0], start, 0)
        lax.fori_loop(0, total[0], wait, 0)


def bwd_kernel(x_ref, c_ref, s_ref, e_ref, up_ref, dn_ref, gt_ref, co_ref):
    xf = x_ref[...].astype(F32)
    n, inv = norm_rows(xf)
    u = n.astype(BF16)
    c = c_ref[...]
    b = dot(u, gt_ref[0])
    db = (gelu_grad(b) * (s_ref[...].astype(F32) * e_ref[...].astype(F32))).astype(BF16)
    du = dot_nt(db, gt_ref[0])
    ff = up_ref.shape[2]
    for k in range(ff // FC):
        w_k = up_ref[0, :, k * FC:(k + 1) * FC]
        a = dot(u, w_k)
        dh = dot_nt(c, dn_ref[0, k * FC:(k + 1) * FC, :]).astype(BF16)
        da = (gelu_grad(a) * dh.astype(F32)).astype(BF16)
        du = du + dot_nt(da, w_k)
    dx = inv * (du - n * jnp.mean(du * n, axis=-1, keepdims=True))
    co_ref[...] = (c.astype(F32) + dx).astype(BF16)


def line_of(row):
    return (row // 8) * (8 * PIECES) + row % 8


def piece_rows(start):
    return pl.ds(start, PIECES, stride=8)


def gather_kernel(steps, line, src_ref, out_ref, table, stage):
    i = pl.program_id(0)
    src_rows = src_ref.shape[1]
    out_rows = out_ref.shape[0]
    span = CH * PIECES

    @pl.when(i < steps)
    def _():
        def widen(t, carry):
            blk = src_ref[0, pl.ds(pl.multiple_of(t * CH, CH), CH), :].astype(F32)
            base = pl.multiple_of((i * src_rows + t * CH) * PIECES, 8)
            for h in range(CH // 8):
                for j in range(PIECES):
                    table[pl.ds(base + (h * PIECES + j) * 8, 8), :] = blk[h * 8:h * 8 + 8, j * 128:j * 128 + 128]
            return carry

        lax.fori_loop(0, src_rows // CH, widen, 0, unroll=2)

    @pl.when(i >= steps)
    def _():
        first = (i - steps) * out_rows

        def pick(t, carry):
            base = pl.multiple_of(t * (8 * PIECES), 8)
            got = [table[piece_rows(line[first + t * 8 + q]), :] for q in range(8)]
            for q, v in enumerate(got):
                stage[piece_rows(base + q), :] = v
            return carry

        lax.fori_loop(0, out_rows // 8, pick, 0, unroll=2)

        def narrow(t, carry):
            base = pl.multiple_of(t * span, 8)
            halves = [
                jnp.concatenate([stage[pl.ds(base + (h * PIECES + j) * 8, 8), :] for j in range(PIECES)], axis=1)
                for h in range(CH // 8)]
            out_ref[pl.ds(pl.multiple_of(t * CH, CH), CH), :] = jnp.concatenate(halves, axis=0).astype(BF16)
            return carry

        lax.fori_loop(0, out_rows // CH, narrow, 0, unroll=2)


def scatter_body(layer, line, count, recv_ref, out_ref, acc, stage, sem):
    i = pl.program_id(0)
    span = 8 * PIECES
    cap = recv_ref.shape[0] // PIECES
    n_lines = acc.shape[0] - PAD

    @pl.when(i == 0)
    def _():
        def clear(t, carry):
            acc[pl.ds(pl.multiple_of(t * span, 8), span), :] = jnp.zeros((span, 128), F32)
            return carry

        lax.fori_loop(0, n_lines // span, clear, 0, unroll=2)

    def load(t, carry):
        at = pl.ds(pl.multiple_of(t * span, 8), span)
        stage[at, :] = recv_ref[at, :]
        return carry

    groups = (count[i] + 7) // 8
    lax.fori_loop(0, groups, load, 0)

    def group(t, carry):
        base = pl.multiple_of(t * span, 8)
        at = [line[i * cap + t * 8 + q] for q in range(8)]
        old = [acc[piece_rows(r), :] for r in at]
        new = [o + stage[piece_rows(base + q), :] for q, o in enumerate(old)]
        for r, v in zip(at, new):
            acc[piece_rows(r), :] = v
        return carry

    lax.fori_loop(0, groups, group, 0)

    @pl.when(i == pl.num_programs(0) - 1)
    def _():
        size = n_lines - span
        cp = pltpu.make_async_copy(acc.at[pl.ds(0, size)], out_ref.at[pl.ds(layer * size, size)], sem)
        cp.start()
        cp.wait()


def scatter_first(layer, line, count, recv_ref, *refs):
    scatter_body(layer, line, count, recv_ref, *refs)


def scatter_next(layer, line, count, recv_ref, _, *refs):
    scatter_body(layer, line, count, recv_ref, *refs)


def to_lines(a):
    n, d = a.shape
    return a.reshape(n // 8, 8, d // 128, 128).transpose(0, 2, 1, 3).reshape(n * d // 128, 128)


def from_lines(a, n, d):
    return a.reshape(n // 8, d // 128, 8, 128).transpose(0, 2, 1, 3).reshape(n, d)


ANY = pl.BlockSpec(memory_space=pl.ANY)


def once(shape, index_map):
    return pl.BlockSpec(shape, index_map, pipeline_mode=pl.Buffered(1))


def params():
    return pltpu.CompilerParams(dimension_semantics=("arbitrary",), vmem_limit_bytes=VMEM_LIMIT)


def cost(flops, nbytes):
    return pl.CostEstimate(flops=int(flops), bytes_accessed=int(nbytes), transcendentals=0)


def solution(mesh):
    group_size = mesh.shape['emb']

    def body(uniq_loc, inv_loc, x_loc, dy_loc, tab_loc, w_up, w_down, w_gate, w_proj):
        layers, shard_rows, d_emb = tab_loc.shape
        n_uniq = uniq_loc.shape[0]
        n_tok, d_model = x_loc.shape
        ff = w_up.shape[2]
        capacity = 2 * n_uniq // group_size
        slots = group_size * capacity
        cap_ch = capacity // CH
        row_chunks = (n_uniq + group_size * CH + WIN) // CH
        n_rows = row_chunks * CH
        my_dev = lax.axis_index('emb')

        iota = jnp.arange(n_tok, dtype=I32)
        low = 64
        hot = (inv_loc[:, None] // low == jnp.arange(n_uniq // low, dtype=I32)[None, :]).astype(BF16)
        grid_ids = uniq_loc.reshape(n_uniq // low, low)
        near = dot(hot, (grid_ids // 256).astype(BF16)) * 256.0 + dot(hot, (grid_ids % 256).astype(BF16))
        mine = inv_loc[:, None] % low == jnp.arange(low, dtype=I32)[None, :]
        tok_id = jnp.sum(jnp.where(mine, near, 0.0), axis=1).astype(I32)
        order = lax.sort(tok_id * n_tok + iota)
        perm = order % n_tok
        sid = order // n_tok
        unperm = lax.sort(perm * n_tok + iota) % n_tok
        is_new = jnp.concatenate([jnp.ones((1,), jnp.bool_), sid[1:] != sid[:-1]])
        rank = jnp.cumsum(is_new.astype(I32)) - 1
        used = lax.sort(jnp.where(is_new, sid, jnp.int32(2 ** 30)))[:n_uniq]
        owners = jnp.arange(group_size, dtype=I32)
        own = sid // shard_rows
        own_hot = own[None, :] == owners[:, None]
        cnt = jnp.sum(jnp.where(own_hot & is_new[None, :], 1, 0), axis=1).astype(I32)
        first = (jnp.cumsum(cnt) - cnt).astype(I32)
        n_ch = (cnt + CH - 1) // CH
        first_ch = (jnp.cumsum(n_ch) - n_ch).astype(I32)
        pos = rank + jnp.sum(jnp.where(own_hot, (first_ch * CH - first)[:, None], 0), axis=0)
        pos = pos.astype(I32)
        wst = pos.reshape(n_tok // SUB, SUB)[:, 0] // CH
        cid = jnp.arange(row_chunks, dtype=I32)[None, :]
        in_own = (cid >= first_ch[:, None]) & (cid < (first_ch + n_ch)[:, None])
        chunk = jnp.sum(jnp.where(in_own, owners[:, None] * cap_ch + cid - first_ch[:, None], 0), axis=0).astype(I32)
        total = jnp.sum(n_ch).astype(I32).reshape(1)
        used_pad = jnp.concatenate([used, jnp.full((capacity,), -1, I32)])
        kk = jnp.arange(capacity, dtype=I32)
        send_ids = jnp.stack([
            jnp.where(kk < cnt[j], lax.dynamic_slice(used_pad, (first[j],), (capacity,)), -1)
            for j in range(group_size)])
        recv_ids = lax.all_to_all(send_ids, 'emb', 0, 0)
        valid = recv_ids >= 0
        local_row = recv_ids - my_dev * shard_rows
        fetch_row = jnp.where(valid, local_row, 0).reshape(-1)
        add_line = line_of(jnp.where(valid, local_row, shard_rows).reshape(-1))
        fetch_line = line_of(fetch_row)
        add_cnt = jnp.sum(valid.astype(I32), axis=1).astype(I32)
        posc = pos.reshape(n_tok, 1)
        posr = pos.reshape(n_tok // SUB, 1, SUB)

        tok_spec = pl.BlockSpec((TB, d_model), lambda i, *_: (i, 0))
        posr_spec = pl.BlockSpec((TB // SUB, 1, SUB), lambda i, *_: (i, 0, 0))
        grid = (n_tok // TB,)
        tok_out = jax.ShapeDtypeStruct((n_tok, d_model), BF16)

        def w_specs(layer, *shapes):
            return [once((1,) + s, lambda i, *_, layer=layer: (layer, 0, 0)) for s in shapes]

        s_up, s_dn, s_sq = (d_model, ff), (ff, d_model), (d_model, d_emb)
        mm = 2.0 * n_tok * d_model * ff
        sq = 2.0 * n_tok * d_model * d_emb

        def forward(layer, x, returned):
            return pl.pallas_call(
                fwd_kernel, out_shape=[tok_out] * 3,
                grid_spec=pltpu.PrefetchScalarGridSpec(
                    num_scalar_prefetch=2, grid=grid,
                    in_specs=[tok_spec, pl.BlockSpec((TB, 1), lambda i, *_: (i, 0)),
                              *w_specs(layer, s_up, s_dn, s_sq, s_sq), ANY],
                    out_specs=[tok_spec] * 3,
                    scratch_shapes=[pltpu.VMEM((n_rows, d_emb), BF16), pltpu.SemaphoreType.DMA]),
                compiler_params=params(), name='fwd',
                cost_estimate=cost(2 * mm + 2 * sq, 3e7),
            )(wst, chunk, x, posc, w_up, w_down, w_gate, w_proj, returned)

        def rowgrad(layer, kernel, operand, c, gate):
            weights = [w_gate] * gate + [w_proj]
            return pl.pallas_call(
                kernel, out_shape=[tok_out, jax.ShapeDtypeStruct((slots, d_emb), F32)],
                grid_spec=pltpu.PrefetchScalarGridSpec(
                    num_scalar_prefetch=3, grid=grid,
                    in_specs=[tok_spec, tok_spec, posr_spec, *w_specs(layer, *[s_sq] * len(weights))],
                    out_specs=[tok_spec, ANY],
                    scratch_shapes=[pltpu.VMEM((n_rows, d_emb), F32), pltpu.SemaphoreType.DMA]),
                compiler_params=params(), name='rowgrad',
                cost_estimate=cost(2 * sq, 3e7),
            )(wst, chunk, total, operand, c, posr, *weights)

        def backward(layer, x, c, s, e):
            return pl.pallas_call(
                bwd_kernel, out_shape=tok_out, grid=grid,
                in_specs=[tok_spec] * 4 + w_specs(layer, s_up, s_dn, s_sq),
                out_specs=tok_spec,
                compiler_params=params(), name='bwd',
                cost_estimate=cost(3 * mm + 2 * sq, 4e7),
            )(x, c, s, e, w_up, w_down, w_gate)

        def scatter(layer, received, grads):
            ins = [pl.BlockSpec((capacity * PIECES, 128), lambda i, *_: (i, 0))]
            args = [to_lines(received)]
            if grads is not None:
                ins.append(ANY)
                args.append(grads)
            return pl.pallas_call(
                functools.partial(scatter_first if grads is None else scatter_next, layer),
                out_shape=jax.ShapeDtypeStruct((layers * shard_rows * PIECES, 128), F32),
                grid_spec=pltpu.PrefetchScalarGridSpec(
                    num_scalar_prefetch=2, grid=(group_size,), in_specs=ins, out_specs=ANY,
                    scratch_shapes=[pltpu.VMEM(((shard_rows + 8) * PIECES + PAD, 128), F32),
                                    pltpu.VMEM((capacity * PIECES + PAD, 128), F32), pltpu.SemaphoreType.DMA]),
                compiler_params=params(), name='scatter',
                input_output_aliases={} if grads is None else {3: 0},
                cost_estimate=cost(1e10, 4e7),
            )(add_line, add_cnt, *args)

        def gather(source, layer, line, src_rows, name):
            n = source.shape[1]
            steps = n // src_rows
            return pl.pallas_call(
                functools.partial(gather_kernel, steps),
                out_shape=jax.ShapeDtypeStruct((line.shape[0], d_emb), BF16),
                grid_spec=pltpu.PrefetchScalarGridSpec(
                    num_scalar_prefetch=1, grid=(steps + line.shape[0] // TB,),
                    in_specs=[pl.BlockSpec((1, src_rows, d_emb),
                                           lambda i, *_: (layer, jnp.minimum(i, steps - 1), 0))],
                    out_specs=pl.BlockSpec((TB, d_emb), lambda i, *_: (jnp.maximum(i - steps, 0), 0)),
                    scratch_shapes=[pltpu.VMEM((n * PIECES + PAD, 128), F32),
                                    pltpu.VMEM((TB * PIECES + PAD, 128), F32)]),
                compiler_params=params(), name=name,
                cost_estimate=cost(1e10, 2e7),
            )(line, source)

        def tok_gather(a, rows, name):
            return gather(a.reshape(1, n_tok, d_model), 0, line_of(rows), n_tok // 4, name)

        def serve(layer, line):
            return gather(tab_loc, layer, line, shard_rows // 3, 'serve').reshape(group_size, capacity, d_emb)

        def exchange(a):
            return lax.all_to_all(a, 'emb', 0, 0)

        served = serve(0, fetch_line)
        got = exchange(served)
        perm, served, later = lax.optimization_barrier((perm, served, fetch_line))
        x = tok_gather(x_loc, perm, 'sort_x')
        c = tok_gather(dy_loc, perm, 'sort_c')
        served = serve(1, later)
        saved_x, saved_e, saved_g = [], [], []
        for layer in range(layers):
            here = got
            if layer + 1 < layers:
                x, c, here, served, later = lax.optimization_barrier((x, c, here, served, later))
                got = exchange(served)
                if layer + 2 < layers:
                    served = serve(layer + 2, later)
            saved_x.append(x)
            x, e, g = forward(layer, x, here.reshape(slots, d_emb))
            saved_e.append(e)
            saved_g.append(g)
        x_out = tok_gather(x, unperm, 'unsort')

        grads = None
        pending = None
        for layer in reversed(range(layers)):
            if layer == layers - 1:
                s, send = rowgrad(layer, rowgrad_top_kernel, saved_x[layer], c, 1)
            else:
                s, send = rowgrad(layer, rowgrad_kernel, saved_g[layer], c, 0)
            got = lax.all_to_all(send.reshape(group_size, capacity, d_emb), 'emb', 0, 0).reshape(slots, d_emb)
            if pending is not None:
                c, pending = lax.optimization_barrier((c, pending))
                grads = scatter(layer + 1, pending, grads)
            if layer > 0:
                c = backward(layer, saved_x[layer], c, s, saved_e[layer])
            pending = got
        grads = scatter(0, pending, grads)
        return x_out, from_lines(grads, layers * shard_rows, d_emb).reshape(layers, shard_rows, d_emb)

    return jax.shard_map(body, mesh=mesh,
                         in_specs=(P('emb'), P('emb'), P('emb', None), P('emb', None), P(None, 'emb', None),
                                   P(), P(), P(), P()),
                         out_specs=(P('emb', None), P(None, 'emb', None)), check_vma=False)
```

```python
import functools

import jax
import jax.numpy as jnp
from jax import lax
from jax.experimental import pallas as pl
from jax.experimental.pallas import tpu as pltpu
from jax.sharding import PartitionSpec as P


EPSILON = 1e-6
BF16 = jnp.bfloat16
F32 = jnp.float32
I32 = jnp.int32

CH = 16
SUB = 256
WIN = 384
TB = 512
PIECES = 6
PAD = 16
FC = 512
VMEM_LIMIT = 60 * 1024 * 1024
G0 = 0.7978845608028654
G1 = G0 * 0.044715


def dot(a, b):
    return jnp.dot(a, b, preferred_element_type=F32)


def dot_nt(a, b):
    return lax.dot_general(a, b, (((1,), (1,)), ((), ())), preferred_element_type=F32)


def gelu(a):
    half = 0.5 * a
    return half * jnp.tanh(a * (G0 + G1 * (a * a))) + half


def gelu_grad(a):
    sq = a * a
    t = jnp.tanh(a * (G0 + G1 * sq))
    return 0.5 * t + 0.5 + (0.5 * a * (1.0 - t * t)) * (G0 + (3.0 * G1) * sq)


def norm_rows(xf):
    inv = lax.rsqrt(jnp.mean(xf * xf, axis=-1, keepdims=True) + EPSILON)
    return xf * inv, inv


def fwd_kernel(wst, chunk, x_ref, posc_ref, up_ref, dn_ref, gt_ref, pj_ref, ret_ref,
               xo_ref, e_ref, g_ref, rows, sem):
    i = pl.program_id(0)
    n_rows = rows.shape[0]

    @pl.when(i == 0)
    def _():
        def start(d, carry):
            src = pl.multiple_of(chunk[d] * CH, CH)
            dst = pl.multiple_of(d * CH, CH)
            pltpu.make_async_copy(ret_ref.at[pl.ds(src, CH)], rows.at[pl.ds(dst, CH)], sem).start()
            return carry

        lax.fori_loop(0, n_rows // CH, start, 0)
        pltpu.make_async_copy(rows, rows, sem).wait()

    tb = x_ref.shape[0]
    xf = x_ref[...].astype(F32)
    u = norm_rows(xf)[0].astype(BF16)
    parts = []
    for q in range(tb // SUB):
        w0 = pl.multiple_of(wst[i * (tb // SUB) + q] * CH, CH)
        col = posc_ref[q * SUB:(q + 1) * SUB, :] - w0
        hot = jnp.where(col == lax.broadcasted_iota(I32, (SUB, WIN), 1), 1.0, 0.0).astype(BF16)
        parts.append(dot(hot, rows[pl.ds(w0, WIN), :]).astype(BF16))
    e = jnp.concatenate(parts, axis=0)
    e_ref[...] = e
    g = gelu(dot(u, gt_ref[0])).astype(BF16)
    g_ref[...] = g
    z = (g.astype(F32) * e.astype(F32)).astype(BF16)
    proj = dot(z, pj_ref[0]).astype(BF16)
    ff = up_ref.shape[2]
    mlp = None
    for k in range(ff // FC):
        h = gelu(dot(u, up_ref[0, :, k * FC:(k + 1) * FC])).astype(BF16)
        part = dot(h, dn_ref[0, k * FC:(k + 1) * FC, :])
        mlp = part if mlp is None else mlp + part
    xo_ref[...] = (xf + mlp.astype(BF16).astype(F32) + proj.astype(F32)).astype(BF16)


def rowgrad_top_kernel(wst, dest, total, x_ref, c_ref, posr_ref, gt_ref, pj_ref, *refs):
    u = norm_rows(x_ref[...].astype(F32))[0].astype(BF16)
    g = gelu(dot(u, gt_ref[0])).astype(BF16)
    rowgrad_body(wst, dest, total, g, c_ref, posr_ref, pj_ref, *refs)


def rowgrad_kernel(wst, dest, total, g_ref, c_ref, posr_ref, pj_ref, *refs):
    rowgrad_body(wst, dest, total, g_ref[...], c_ref, posr_ref, pj_ref, *refs)


def rowgrad_body(wst, dest, total, g, c_ref, posr_ref, pj_ref, s_ref, base_ref, over_ref, rest_ref, acc, sem):
    i = pl.program_id(0)
    last = pl.num_programs(0) - 1

    @pl.when(i == 0)
    def _():
        acc[...] = jnp.zeros_like(acc)

    tb = c_ref.shape[0]
    s = dot_nt(c_ref[...], pj_ref[0]).astype(BF16)
    s_ref[...] = s
    k = g.astype(F32) * s.astype(F32)
    hi = k.astype(BF16)
    lo = (k - hi.astype(F32)).astype(BF16)
    for q in range(tb // SUB):
        w0 = pl.multiple_of(wst[i * (tb // SUB) + q] * CH, CH)
        row = posr_ref[q] - w0
        hot = jnp.where(row == lax.broadcasted_iota(I32, (WIN, SUB), 0), 1.0, 0.0).astype(BF16)
        sl = slice(q * SUB, (q + 1) * SUB)
        acc[pl.ds(w0, WIN), :] += dot(hot, hi[sl]) + dot(hot, lo[sl])

    @pl.when(i == last)
    def _():
        edges = [0]
        for ref in (base_ref, over_ref, rest_ref):
            edges.append(edges[-1] + ref.shape[0] // CH)

        def start(d, carry):
            src = acc.at[pl.ds(pl.multiple_of(d * CH, CH), CH)]
            to = dest[d]
            for ref, low, high in zip((base_ref, over_ref, rest_ref), edges, edges[1:]):
                @pl.when((to >= low) & (to < high))
                def _():
                    dst = ref.at[pl.ds(pl.multiple_of((to - low) * CH, CH), CH)]
                    pltpu.make_async_copy(src, dst, sem).start()
            return carry

        def wait(d, carry):
            pltpu.make_async_copy(acc.at[pl.ds(0, CH)], base_ref.at[pl.ds(0, CH)], sem).wait()
            return carry

        lax.fori_loop(0, total[0], start, 0)
        lax.fori_loop(0, total[0], wait, 0)


def bwd_kernel(x_ref, c_ref, s_ref, e_ref, up_ref, dn_ref, gt_ref, co_ref):
    xf = x_ref[...].astype(F32)
    n, inv = norm_rows(xf)
    u = n.astype(BF16)
    c = c_ref[...]
    b = dot(u, gt_ref[0])
    db = (gelu_grad(b) * (s_ref[...].astype(F32) * e_ref[...].astype(F32))).astype(BF16)
    du = dot_nt(db, gt_ref[0])
    ff = up_ref.shape[2]
    for k in range(ff // FC):
        w_k = up_ref[0, :, k * FC:(k + 1) * FC]
        a = dot(u, w_k)
        dh = dot_nt(c, dn_ref[0, k * FC:(k + 1) * FC, :]).astype(BF16)
        da = (gelu_grad(a) * dh.astype(F32)).astype(BF16)
        du = du + dot_nt(da, w_k)
    dx = inv * (du - n * jnp.mean(du * n, axis=-1, keepdims=True))
    co_ref[...] = (c.astype(F32) + dx).astype(BF16)


def line_of(row):
    return (row // 8) * (8 * PIECES) + row % 8


def piece_rows(start):
    return pl.ds(start, PIECES, stride=8)


def gather_kernel(steps, line, src_ref, out_ref, table, stage):
    i = pl.program_id(0)
    src_rows = src_ref.shape[1]
    out_rows = out_ref.shape[0]
    span = CH * PIECES

    @pl.when(i < steps)
    def _():
        def widen(t, carry):
            blk = src_ref[0, pl.ds(pl.multiple_of(t * CH, CH), CH), :].astype(F32)
            base = pl.multiple_of((i * src_rows + t * CH) * PIECES, 8)
            for h in range(CH // 8):
                for j in range(PIECES):
                    table[pl.ds(base + (h * PIECES + j) * 8, 8), :] = blk[h * 8:h * 8 + 8, j * 128:j * 128 + 128]
            return carry

        lax.fori_loop(0, src_rows // CH, widen, 0, unroll=2)

    @pl.when(i >= steps)
    def _():
        first = (i - steps) * out_rows

        def pick(t, carry):
            base = pl.multiple_of(t * (8 * PIECES), 8)
            got = [table[piece_rows(line[first + t * 8 + q]), :] for q in range(8)]
            for q, v in enumerate(got):
                stage[piece_rows(base + q), :] = v
            return carry

        lax.fori_loop(0, out_rows // 8, pick, 0, unroll=2)

        def narrow(t, carry):
            base = pl.multiple_of(t * span, 8)
            halves = [
                jnp.concatenate([stage[pl.ds(base + (h * PIECES + j) * 8, 8), :] for j in range(PIECES)], axis=1)
                for h in range(CH // 8)]
            out_ref[pl.ds(pl.multiple_of(t * CH, CH), CH), :] = jnp.concatenate(halves, axis=0).astype(BF16)
            return carry

        lax.fori_loop(0, out_rows // CH, narrow, 0, unroll=2)


def add_rows(line, at, groups, recv_ref, first, acc, stage):
    span = 8 * PIECES

    def load(t, carry):
        src = pl.ds(pl.multiple_of(first + t * span, 8), span)
        stage[pl.ds(pl.multiple_of(t * span, 8), span), :] = recv_ref[src, :]
        return carry

    def group(t, carry):
        base = pl.multiple_of(t * span, 8)
        to = [line[at + t * 8 + q] for q in range(8)]
        old = [acc[piece_rows(r), :] for r in to]
        new = [o + stage[piece_rows(base + q), :] for q, o in enumerate(old)]
        for r, v in zip(to, new):
            acc[piece_rows(r), :] = v
        return carry

    lax.fori_loop(0, groups, load, 0)
    lax.fori_loop(0, groups, group, 0)


def store_layer(layer, out_ref, acc, sem, back=False):
    size = acc.shape[0] - PAD - 8 * PIECES
    ends = acc.at[pl.ds(0, size)], out_ref.at[pl.ds(layer * size, size)]
    cp = pltpu.make_async_copy(ends[1], ends[0], sem) if back else pltpu.make_async_copy(*ends, sem)
    cp.start()
    cp.wait()


def scatter_kernel(layer, line, n_base, n_over, at_over, base_ref, over_ref, *refs):
    out_ref, acc, stage, sem = refs[-4:]
    i = pl.program_id(0)
    span = 8 * PIECES
    cap = base_ref.shape[0] // PIECES + over_ref.shape[0] // PIECES

    @pl.when(i == 0)
    def _():
        def clear(t, carry):
            acc[pl.ds(pl.multiple_of(t * span, 8), span), :] = jnp.zeros((span, 128), F32)
            return carry

        lax.fori_loop(0, (acc.shape[0] - PAD) // span, clear, 0, unroll=2)

    add_rows(line, i * cap, (n_base[i] + 7) // 8, base_ref, 0, acc, stage)
    add_rows(line, i * cap + cap // 2, (n_over[i] + 7) // 8, over_ref, at_over[i] * (CH * PIECES), acc, stage)

    @pl.when(i == pl.num_programs(0) - 1)
    def _():
        store_layer(layer, out_ref, acc, sem)


def rest_kernel(layer, line, n_rest, rest_ref, _, out_ref, acc, stage, sem):
    i = pl.program_id(0)
    cap = 2 * rest_ref.shape[0] // PIECES

    @pl.when(i == 0)
    def _():
        store_layer(layer, out_ref, acc, sem, back=True)

    add_rows(line, i * cap + cap // 2, (n_rest[i] + 7) // 8, rest_ref, 0, acc, stage)

    @pl.when(i == pl.num_programs(0) - 1)
    def _():
        store_layer(layer, out_ref, acc, sem)


def to_lines(a):
    n, d = a.shape
    return a.reshape(n // 8, 8, d // 128, 128).transpose(0, 2, 1, 3).reshape(n * d // 128, 128)


def from_lines(a, n, d):
    return a.reshape(n // 8, d // 128, 8, 128).transpose(0, 2, 1, 3).reshape(n, d)


ANY = pl.BlockSpec(memory_space=pl.ANY)


def once(shape, index_map):
    return pl.BlockSpec(shape, index_map, pipeline_mode=pl.Buffered(1))


def params():
    return pltpu.CompilerParams(dimension_semantics=("arbitrary",), vmem_limit_bytes=VMEM_LIMIT)


def cost(flops, nbytes):
    return pl.CostEstimate(flops=int(flops), bytes_accessed=int(nbytes), transcendentals=0)


def solution(mesh):
    group_size = mesh.shape['emb']

    def body(uniq_loc, inv_loc, x_loc, dy_loc, tab_loc, w_up, w_down, w_gate, w_proj):
        layers, shard_rows, d_emb = tab_loc.shape
        n_uniq = uniq_loc.shape[0]
        n_tok, d_model = x_loc.shape
        ff = w_up.shape[2]
        capacity = 2 * n_uniq // group_size
        slots = group_size * capacity
        cap_ch = capacity // CH
        row_chunks = (n_uniq + group_size * CH + WIN) // CH
        n_rows = row_chunks * CH
        my_dev = lax.axis_index('emb')

        iota = jnp.arange(n_tok, dtype=I32)
        low = 64
        hot = (inv_loc[:, None] // low == jnp.arange(n_uniq // low, dtype=I32)[None, :]).astype(BF16)
        grid_ids = uniq_loc.reshape(n_uniq // low, low)
        near = dot(hot, (grid_ids // 256).astype(BF16)) * 256.0 + dot(hot, (grid_ids % 256).astype(BF16))
        mine = inv_loc[:, None] % low == jnp.arange(low, dtype=I32)[None, :]
        tok_id = jnp.sum(jnp.where(mine, near, 0.0), axis=1).astype(I32)
        order = lax.sort(tok_id * n_tok + iota)
        perm = order % n_tok
        sid = order // n_tok
        unperm = lax.sort(perm * n_tok + iota) % n_tok
        is_new = jnp.concatenate([jnp.ones((1,), jnp.bool_), sid[1:] != sid[:-1]])
        rank = jnp.cumsum(is_new.astype(I32)) - 1
        used = lax.sort(jnp.where(is_new, sid, jnp.int32(2 ** 30)))[:n_uniq]
        owners = jnp.arange(group_size, dtype=I32)
        own = sid // shard_rows
        own_hot = own[None, :] == owners[:, None]
        cnt = jnp.sum(jnp.where(own_hot & is_new[None, :], 1, 0), axis=1).astype(I32)
        first = (jnp.cumsum(cnt) - cnt).astype(I32)
        n_ch = (cnt + CH - 1) // CH
        first_ch = (jnp.cumsum(n_ch) - n_ch).astype(I32)
        pos = rank + jnp.sum(jnp.where(own_hot, (first_ch * CH - first)[:, None], 0), axis=0)
        pos = pos.astype(I32)
        wst = pos.reshape(n_tok // SUB, SUB)[:, 0] // CH
        cid = jnp.arange(row_chunks, dtype=I32)[None, :]
        in_own = (cid >= first_ch[:, None]) & (cid < (first_ch + n_ch)[:, None])
        chunk = jnp.sum(jnp.where(in_own, owners[:, None] * cap_ch + cid - first_ch[:, None], 0), axis=0).astype(I32)
        half_ch = cap_ch // 2
        over_ch = jnp.maximum(n_ch - half_ch, 0)
        over_first = (jnp.cumsum(over_ch) - over_ch).astype(I32)
        fits = over_first + over_ch <= half_ch
        k_ch = cid - first_ch[:, None]
        over_dest = jnp.where(fits, group_size * half_ch + over_first - half_ch,
                              (group_size + 1) * half_ch + (owners - 1) * half_ch)
        dest = jnp.where(k_ch < half_ch, owners[:, None] * half_ch + k_ch, over_dest[:, None] + k_ch)
        dest = jnp.sum(jnp.where(in_own, dest, 0), axis=0).astype(I32)
        unfit = jnp.any(~fits).astype(I32)
        total = jnp.sum(n_ch).astype(I32).reshape(1)
        used_pad = jnp.concatenate([used, jnp.full((capacity,), -1, I32)])
        kk = jnp.arange(capacity, dtype=I32)
        send_ids = jnp.stack([
            jnp.where(kk < cnt[j], lax.dynamic_slice(used_pad, (first[j],), (capacity,)), -1)
            for j in range(group_size)])
        notes = jnp.where(jnp.arange(128)[None, :] == 0, over_first[:, None], unfit)
        mail = lax.all_to_all(jnp.concatenate([send_ids, notes], axis=1), 'emb', 0, 0)
        recv_ids = mail[:, :capacity]
        valid = recv_ids >= 0
        local_row = recv_ids - my_dev * shard_rows
        fetch_row = jnp.where(valid, local_row, 0).reshape(-1)
        add_line = line_of(jnp.where(valid, local_row, shard_rows).reshape(-1))
        fetch_line = line_of(fetch_row)
        recv_cnt = jnp.sum(valid.astype(I32), axis=1).astype(I32)
        half = capacity // 2
        n_base = jnp.minimum(recv_cnt, half)
        beyond = jnp.maximum(recv_cnt - half, 0)
        at_over = mail[:, capacity]
        fitted = at_over + (beyond + CH - 1) // CH <= half_ch
        n_over = jnp.where(fitted, beyond, 0)
        at_over = jnp.where(fitted, at_over, 0)
        n_rest = jnp.where(fitted, 0, beyond)
        any_rest = jnp.max(mail[:, capacity + 1])
        posc = pos.reshape(n_tok, 1)
        posr = pos.reshape(n_tok // SUB, 1, SUB)

        tok_spec = pl.BlockSpec((TB, d_model), lambda i, *_: (i, 0))
        posr_spec = pl.BlockSpec((TB // SUB, 1, SUB), lambda i, *_: (i, 0, 0))
        grid = (n_tok // TB,)
        tok_out = jax.ShapeDtypeStruct((n_tok, d_model), BF16)

        def w_specs(layer, *shapes):
            return [once((1,) + s, lambda i, *_, layer=layer: (layer, 0, 0)) for s in shapes]

        s_up, s_dn, s_sq = (d_model, ff), (ff, d_model), (d_model, d_emb)
        mm = 2.0 * n_tok * d_model * ff
        sq = 2.0 * n_tok * d_model * d_emb

        def forward(layer, x, returned):
            return pl.pallas_call(
                fwd_kernel, out_shape=[tok_out] * 3,
                grid_spec=pltpu.PrefetchScalarGridSpec(
                    num_scalar_prefetch=2, grid=grid,
                    in_specs=[tok_spec, pl.BlockSpec((TB, 1), lambda i, *_: (i, 0)),
                              *w_specs(layer, s_up, s_dn, s_sq, s_sq), ANY],
                    out_specs=[tok_spec] * 3,
                    scratch_shapes=[pltpu.VMEM((n_rows, d_emb), BF16), pltpu.SemaphoreType.DMA]),
                compiler_params=params(), name='fwd',
                cost_estimate=cost(2 * mm + 2 * sq, 3e7),
            )(wst, chunk, x, posc, w_up, w_down, w_gate, w_proj, returned)

        def rowgrad(layer, kernel, operand, c, gate):
            weights = [w_gate] * gate + [w_proj]
            return pl.pallas_call(
                kernel, out_shape=[tok_out] + [jax.ShapeDtypeStruct((r, d_emb), F32) for r in (slots // 2, half, slots // 2)],
                grid_spec=pltpu.PrefetchScalarGridSpec(
                    num_scalar_prefetch=3, grid=grid,
                    in_specs=[tok_spec, tok_spec, posr_spec, *w_specs(layer, *[s_sq] * len(weights))],
                    out_specs=[tok_spec, ANY, ANY, ANY],
                    scratch_shapes=[pltpu.VMEM((n_rows, d_emb), F32), pltpu.SemaphoreType.DMA]),
                compiler_params=params(), name='rowgrad',
                cost_estimate=cost(2 * sq, 3e7),
            )(wst, dest, total, operand, c, posr, *weights)

        def backward(layer, x, c, s, e):
            return pl.pallas_call(
                bwd_kernel, out_shape=tok_out, grid=grid,
                in_specs=[tok_spec] * 4 + w_specs(layer, s_up, s_dn, s_sq),
                out_specs=tok_spec,
                compiler_params=params(), name='bwd',
                cost_estimate=cost(3 * mm + 2 * sq, 4e7),
            )(x, c, s, e, w_up, w_down, w_gate)

        half_spec = pl.BlockSpec((half * PIECES, 128), lambda i, *_: (i, 0))
        acc_scratch = [pltpu.VMEM(((shard_rows + 8) * PIECES + PAD, 128), F32),
                       pltpu.VMEM((half * PIECES + PAD, 128), F32), pltpu.SemaphoreType.DMA]
        lines_out = jax.ShapeDtypeStruct((layers * shard_rows * PIECES, 128), F32)

        def scatter(layer, received, grads):
            prior = [] if grads is None else [grads]
            return pl.pallas_call(
                functools.partial(scatter_kernel, layer), out_shape=lines_out,
                grid_spec=pltpu.PrefetchScalarGridSpec(
                    num_scalar_prefetch=4, grid=(group_size,),
                    in_specs=[half_spec, half_spec] + [ANY] * len(prior), out_specs=ANY, scratch_shapes=acc_scratch),
                compiler_params=params(), name='scatter',
                input_output_aliases={6: 0} if prior else {},
                cost_estimate=cost(1e10, 4e7),
            )(add_line, n_base, n_over, at_over, to_lines(received[0]), to_lines(received[1]), *prior)

        def scatter_rest(layer, received, grads):
            return pl.pallas_call(
                functools.partial(rest_kernel, layer), out_shape=lines_out,
                grid_spec=pltpu.PrefetchScalarGridSpec(
                    num_scalar_prefetch=2, grid=(group_size,),
                    in_specs=[half_spec, ANY], out_specs=ANY, scratch_shapes=acc_scratch),
                compiler_params=params(), name='scatter_rest', input_output_aliases={3: 0},
                cost_estimate=cost(1e10, 4e7),
            )(add_line, n_rest, to_lines(received), grads)

        def send_home(a):
            return exchange(a.reshape(group_size, half, d_emb)).reshape(slots // 2, d_emb)

        def gather(source, layer, line, src_rows):
            n = source.shape[1]
            steps = n // src_rows
            return pl.pallas_call(
                functools.partial(gather_kernel, steps),
                out_shape=jax.ShapeDtypeStruct((line.shape[0], d_emb), BF16),
                grid_spec=pltpu.PrefetchScalarGridSpec(
                    num_scalar_prefetch=1, grid=(steps + line.shape[0] // TB,),
                    in_specs=[pl.BlockSpec((1, src_rows, d_emb),
                                           lambda i, *_: (layer, jnp.minimum(i, steps - 1), 0))],
                    out_specs=pl.BlockSpec((TB, d_emb), lambda i, *_: (jnp.maximum(i - steps, 0), 0)),
                    scratch_shapes=[pltpu.VMEM((n * PIECES + PAD, 128), F32),
                                    pltpu.VMEM((TB * PIECES + PAD, 128), F32)]),
                compiler_params=params(),
                cost_estimate=cost(1e10, 2e7),
            )(line, source)

        def tok_gather(a, rows):
            return gather(a.reshape(1, n_tok, d_model), 0, line_of(rows), n_tok // 4)

        def serve(layer, line):
            return gather(tab_loc, layer, line, shard_rows // 3).reshape(group_size, capacity, d_emb)

        def exchange(a):
            return lax.all_to_all(a, 'emb', 0, 0)

        served = serve(0, fetch_line)
        got = exchange(served)
        perm, served, later = lax.optimization_barrier((perm, served, fetch_line))
        x = tok_gather(x_loc, perm)
        c = tok_gather(dy_loc, perm)
        served = serve(1, later)
        saved_x, saved_e, saved_g = [], [], []
        for layer in range(layers):
            here = got
            if layer + 1 < layers:
                x, c, here, served, later = lax.optimization_barrier((x, c, here, served, later))
                got = exchange(served)
                if layer + 2 < layers:
                    served = serve(layer + 2, later)
            saved_x.append(x)
            x, e, g = forward(layer, x, here.reshape(slots, d_emb))
            saved_e.append(e)
            saved_g.append(g)
        x_out = tok_gather(x, unperm)

        grads = None
        pending = None
        rests = []
        for layer in reversed(range(layers)):
            if layer == layers - 1:
                s, base, over, rest = rowgrad(layer, rowgrad_top_kernel, saved_x[layer], c, 1)
            else:
                s, base, over, rest = rowgrad(layer, rowgrad_kernel, saved_g[layer], c, 0)
            rests.append((layer, rest))
            base = send_home(base)
            got = base, lax.all_gather(over, 'emb', axis=0, tiled=True)
            if pending is not None:
                c, pending = lax.optimization_barrier((c, pending))
                grads = scatter(layer + 1, pending, grads)
            if layer > 0:
                c = backward(layer, saved_x[layer], c, s, saved_e[layer])
            pending = got
        grads = scatter(0, pending, grads)

        def add_rest(state):
            left, acc = state
            for layer, rest in rests:
                rest, left = lax.optimization_barrier((rest, left))
                acc = scatter_rest(layer, send_home(rest), acc)
            return left - 1, acc

        grads = lax.while_loop(lambda state: state[0] > 0, add_rest, (any_rest, grads))[1]
        return x_out, from_lines(grads, layers * shard_rows, d_emb).reshape(layers, shard_rows, d_emb)

    return jax.shard_map(body, mesh=mesh,
                         in_specs=(P('emb'), P('emb'), P('emb', None), P('emb', None), P(None, 'emb', None),
                                   P(), P(), P(), P()),
                         out_specs=(P('emb', None), P(None, 'emb', None)), check_vma=False)
```

```python
import functools

import jax
import jax.numpy as jnp
from jax import lax
from jax.experimental import pallas as pl
from jax.experimental.pallas import tpu as pltpu
from jax.sharding import PartitionSpec as P


EPSILON = 1e-6
BF16 = jnp.bfloat16
F32 = jnp.float32
I32 = jnp.int32

CH = 16
SUB = 256
WIN = 384
TB = 512
PIECES = 6
PAD = 16
FC = 512
VMEM_LIMIT = 60 * 1024 * 1024
G0 = 0.7978845608028654
G1 = G0 * 0.044715


def dot(a, b):
    return jnp.dot(a, b, preferred_element_type=F32)


def dot_nt(a, b):
    return lax.dot_general(a, b, (((1,), (1,)), ((), ())), preferred_element_type=F32)


def gelu(a):
    half = 0.5 * a
    return half * jnp.tanh(a * (G0 + G1 * (a * a))) + half


def gelu_grad(a):
    sq = a * a
    t = jnp.tanh(a * (G0 + G1 * sq))
    return 0.5 * t + 0.5 + (0.5 * a * (1.0 - t * t)) * (G0 + (3.0 * G1) * sq)


def norm_rows(xf):
    inv = lax.rsqrt(jnp.mean(xf * xf, axis=-1, keepdims=True) + EPSILON)
    return xf * inv, inv


def fwd_kernel(wst, chunk, x_ref, posc_ref, up_ref, dn_ref, gt_ref, pj_ref, ret_ref,
               xo_ref, e_ref, g_ref, rows, sem):
    i = pl.program_id(0)
    n_rows = rows.shape[0]

    @pl.when(i == 0)
    def _():
        def start(d, carry):
            src = pl.multiple_of(chunk[d] * CH, CH)
            dst = pl.multiple_of(d * CH, CH)
            pltpu.make_async_copy(ret_ref.at[pl.ds(src, CH)], rows.at[pl.ds(dst, CH)], sem).start()
            return carry

        lax.fori_loop(0, n_rows // CH, start, 0)
        pltpu.make_async_copy(rows, rows, sem).wait()

    tb = x_ref.shape[0]
    xf = x_ref[...].astype(F32)
    u = norm_rows(xf)[0].astype(BF16)
    parts = []
    for q in range(tb // SUB):
        w0 = pl.multiple_of(wst[i * (tb // SUB) + q] * CH, CH)
        col = posc_ref[q * SUB:(q + 1) * SUB, :] - w0
        hot = jnp.where(col == lax.broadcasted_iota(I32, (SUB, WIN), 1), 1.0, 0.0).astype(BF16)
        parts.append(dot(hot, rows[pl.ds(w0, WIN), :]).astype(BF16))
    e = jnp.concatenate(parts, axis=0)
    e_ref[...] = e
    g = gelu(dot(u, gt_ref[0])).astype(BF16)
    g_ref[...] = g
    z = (g.astype(F32) * e.astype(F32)).astype(BF16)
    proj = dot(z, pj_ref[0]).astype(BF16)
    ff = up_ref.shape[2]
    mlp = None
    for k in range(ff // FC):
        h = gelu(dot(u, up_ref[0, :, k * FC:(k + 1) * FC])).astype(BF16)
        part = dot(h, dn_ref[0, k * FC:(k + 1) * FC, :])
        mlp = part if mlp is None else mlp + part
    xo_ref[...] = (xf + mlp.astype(BF16).astype(F32) + proj.astype(F32)).astype(BF16)


def rowgrad_top_kernel(wst, dest, total, x_ref, c_ref, posr_ref, gt_ref, pj_ref, *refs):
    u = norm_rows(x_ref[...].astype(F32))[0].astype(BF16)
    g = gelu(dot(u, gt_ref[0])).astype(BF16)
    rowgrad_body(wst, dest, total, g, c_ref[...], posr_ref, pj_ref, *refs)


def rowgrad_body(wst, dest, total, g, c, posr_ref, pj_ref, s_ref, base_ref, over_ref, rest_ref, acc, sem):
    i = pl.program_id(0)
    last = pl.num_programs(0) - 1

    @pl.when(i == 0)
    def _():
        acc[...] = jnp.zeros_like(acc)

    tb = c.shape[0]
    s = dot_nt(c, pj_ref[0]).astype(BF16)
    s_ref[...] = s
    k = g.astype(F32) * s.astype(F32)
    hi = k.astype(BF16)
    lo = (k - hi.astype(F32)).astype(BF16)
    for q in range(tb // SUB):
        w0 = pl.multiple_of(wst[i * (tb // SUB) + q] * CH, CH)
        row = posr_ref[q] - w0
        hot = jnp.where(row == lax.broadcasted_iota(I32, (WIN, SUB), 0), 1.0, 0.0).astype(BF16)
        sl = slice(q * SUB, (q + 1) * SUB)
        acc[pl.ds(w0, WIN), :] += dot(hot, hi[sl]) + dot(hot, lo[sl])

    @pl.when(i == last)
    def _():
        edges = [0]
        for ref in (base_ref, over_ref, rest_ref):
            edges.append(edges[-1] + ref.shape[0] // CH)

        def start(d, carry):
            src = acc.at[pl.ds(pl.multiple_of(d * CH, CH), CH)]
            to = dest[d]
            for ref, low, high in zip((base_ref, over_ref, rest_ref), edges, edges[1:]):
                @pl.when((to >= low) & (to < high))
                def _():
                    dst = ref.at[pl.ds(pl.multiple_of((to - low) * CH, CH), CH)]
                    pltpu.make_async_copy(src, dst, sem).start()
            return carry

        def wait(d, carry):
            pltpu.make_async_copy(acc.at[pl.ds(0, CH)], base_ref.at[pl.ds(0, CH)], sem).wait()
            return carry

        lax.fori_loop(0, total[0], start, 0)
        lax.fori_loop(0, total[0], wait, 0)


def bwd_kernel(wst, dest, total, x_ref, c_ref, s_ref, e_ref, up_ref, dn_ref, gt_ref, g_ref, posr_ref, pj_ref,
               co_ref, *refs):
    xf = x_ref[...].astype(F32)
    n, inv = norm_rows(xf)
    u = n.astype(BF16)
    c = c_ref[...]
    b = dot(u, gt_ref[0])
    db = (gelu_grad(b) * (s_ref[...].astype(F32) * e_ref[...].astype(F32))).astype(BF16)
    du = dot_nt(db, gt_ref[0])
    ff = up_ref.shape[2]
    for k in range(ff // FC):
        w_k = up_ref[0, :, k * FC:(k + 1) * FC]
        a = dot(u, w_k)
        dh = dot_nt(c, dn_ref[0, k * FC:(k + 1) * FC, :]).astype(BF16)
        da = (gelu_grad(a) * dh.astype(F32)).astype(BF16)
        du = du + dot_nt(da, w_k)
    dx = inv * (du - n * jnp.mean(du * n, axis=-1, keepdims=True))
    down = (c.astype(F32) + dx).astype(BF16)
    co_ref[...] = down
    rowgrad_body(wst, dest, total, g_ref[...], down, posr_ref, pj_ref, *refs)


def line_of(row):
    return (row // 8) * (8 * PIECES) + row % 8


def piece_rows(start):
    return pl.ds(start, PIECES, stride=8)


def gather_kernel(steps, line, src_ref, out_ref, table, stage):
    i = pl.program_id(0)
    src_rows = src_ref.shape[1]
    out_rows = out_ref.shape[0]
    span = CH * PIECES

    @pl.when(i < steps)
    def _():
        def widen(t, carry):
            blk = src_ref[0, pl.ds(pl.multiple_of(t * CH, CH), CH), :].astype(F32)
            base = pl.multiple_of((i * src_rows + t * CH) * PIECES, 8)
            for h in range(CH // 8):
                for j in range(PIECES):
                    table[pl.ds(base + (h * PIECES + j) * 8, 8), :] = blk[h * 8:h * 8 + 8, j * 128:j * 128 + 128]
            return carry

        lax.fori_loop(0, src_rows // CH, widen, 0, unroll=2)

    @pl.when(i >= steps)
    def _():
        first = (i - steps) * out_rows

        def pick(t, carry):
            base = pl.multiple_of(t * (8 * PIECES), 8)
            got = [table[piece_rows(line[first + t * 8 + q]), :] for q in range(8)]
            for q, v in enumerate(got):
                stage[piece_rows(base + q), :] = v
            return carry

        lax.fori_loop(0, out_rows // 8, pick, 0, unroll=2)

        def narrow(t, carry):
            base = pl.multiple_of(t * span, 8)
            halves = [
                jnp.concatenate([stage[pl.ds(base + (h * PIECES + j) * 8, 8), :] for j in range(PIECES)], axis=1)
                for h in range(CH // 8)]
            out_ref[pl.ds(pl.multiple_of(t * CH, CH), CH), :] = jnp.concatenate(halves, axis=0).astype(BF16)
            return carry

        lax.fori_loop(0, out_rows // CH, narrow, 0, unroll=2)


def add_rows(line, at, groups, recv_ref, first, acc, offset, stage):
    span = 8 * PIECES
    inside = jnp.maximum((recv_ref.shape[0] - first) // span - 1, 0)

    def add(t, read):
        to = [line[at + t * 8 + q] + offset for q in range(8)]
        new = [acc[piece_rows(r), :] + read(q) for q, r in enumerate(to)]
        for r, v in zip(to, new):
            acc[piece_rows(r), :] = v

    def group(t, carry):
        base = pl.multiple_of(first + t * span, 8)
        add(t, lambda q: recv_ref[piece_rows(base + q), :])
        return carry

    lax.fori_loop(0, jnp.minimum(groups, inside), group, 0)

    @pl.when(groups > inside)
    def _():
        stage[0:span, :] = recv_ref[recv_ref.shape[0] - span:, :]
        add(inside, lambda q: stage[piece_rows(q), :])


def clear_lines(acc, first, size):
    span = 8 * PIECES

    def clear(t, carry):
        acc[pl.ds(pl.multiple_of(first + t * span, 8), span), :] = jnp.zeros((span, 128), F32)
        return carry

    lax.fori_loop(0, size // span, clear, 0, unroll=2)


def store_layer(layer, out_ref, acc, sem, back=False):
    size = acc.shape[0] - PAD - 8 * PIECES
    ends = acc.at[pl.ds(0, size)], out_ref.at[pl.ds(layer * size, size)]
    cp = pltpu.make_async_copy(ends[1], ends[0], sem) if back else pltpu.make_async_copy(*ends, sem)
    cp.start()
    cp.wait()


def scatter_kernel(layer, line, n_base, n_over, at_over, base_ref, over_ref, _, out_ref, acc, stage, sem):
    i = pl.program_id(0)
    half = base_ref.shape[0] // PIECES

    @pl.when(i == 0)
    def _():
        clear_lines(acc, 0, acc.shape[0] - PAD)

    add_rows(line, 2 * i * half, (n_base[i] + 7) // 8, base_ref, 0, acc, 0, stage)
    add_rows(line, (2 * i + 1) * half, (n_over[i] + 7) // 8, over_ref, at_over[i] * (CH * PIECES), acc, 0, stage)

    @pl.when(i == pl.num_programs(0) - 1)
    def _():
        store_layer(layer, out_ref, acc, sem)


def scatter_many_kernel(order, line, n_base, n_over, at_over, *refs):
    n = len(order)
    recv, (out_ref, acc, stage, sem) = refs[:2 * n], refs[2 * n:]
    p, i = pl.program_id(0), pl.program_id(1)
    last = pl.num_programs(1) - 1
    half = recv[0].shape[0] // PIECES
    slot_lines = (acc.shape[0] - PAD) // 2
    size = slot_lines - 8 * PIECES
    offset = lax.rem(p, 2) * slot_lines

    def store(at):
        slot = at % 2
        return pltpu.make_async_copy(acc.at[pl.ds(slot * slot_lines, size)],
                                     out_ref.at[pl.ds(order[at] * size, size)], sem.at[slot])

    for at in range(n):
        @pl.when(p == at)
        def _():
            @pl.when(i == 0)
            def _():
                if at >= 2:
                    store(at - 2).wait()
                clear_lines(acc, (at % 2) * slot_lines, slot_lines)

            base_ref, over_ref = recv[2 * at], recv[2 * at + 1]
            add_rows(line, 2 * i * half, (n_base[i] + 7) // 8, base_ref, 0, acc, offset, stage)
            add_rows(line, (2 * i + 1) * half, (n_over[i] + 7) // 8, over_ref, at_over[i] * (CH * PIECES), acc, offset,
                     stage)

            @pl.when(i == last)
            def _():
                store(at).start()
                if at == n - 1:
                    if n > 1:
                        store(at - 1).wait()
                    store(at).wait()


def rest_kernel(layer, line, n_rest, rest_ref, _, out_ref, acc, stage, sem):
    i = pl.program_id(0)
    cap = 2 * rest_ref.shape[0] // PIECES

    @pl.when(i == 0)
    def _():
        store_layer(layer, out_ref, acc, sem, back=True)

    add_rows(line, i * cap + cap // 2, (n_rest[i] + 7) // 8, rest_ref, 0, acc, 0, stage)

    @pl.when(i == pl.num_programs(0) - 1)
    def _():
        store_layer(layer, out_ref, acc, sem)


def to_lines(a):
    n, d = a.shape
    return a.reshape(n // 8, 8, d // 128, 128).transpose(0, 2, 1, 3).reshape(n * d // 128, 128)


def from_lines(a, n, d):
    return a.reshape(n // 8, d // 128, 8, 128).transpose(0, 2, 1, 3).reshape(n, d)


ANY = pl.BlockSpec(memory_space=pl.ANY)


def once(shape, index_map):
    return pl.BlockSpec(shape, index_map, pipeline_mode=pl.Buffered(1))


def params():
    return pltpu.CompilerParams(dimension_semantics=("arbitrary",), vmem_limit_bytes=VMEM_LIMIT)


def cost(flops, nbytes):
    return pl.CostEstimate(flops=int(flops), bytes_accessed=int(nbytes), transcendentals=0)


def solution(mesh):
    group_size = mesh.shape['emb']

    def body(uniq_loc, inv_loc, x_loc, dy_loc, tab_loc, w_up, w_down, w_gate, w_proj):
        layers, shard_rows, d_emb = tab_loc.shape
        n_uniq = uniq_loc.shape[0]
        n_tok, d_model = x_loc.shape
        ff = w_up.shape[2]
        capacity = 2 * n_uniq // group_size
        slots = group_size * capacity
        cap_ch = capacity // CH
        row_chunks = (n_uniq + group_size * CH + WIN) // CH
        n_rows = row_chunks * CH
        my_dev = lax.axis_index('emb')

        iota = jnp.arange(n_tok, dtype=I32)
        low = 64
        hot = (inv_loc[:, None] // low == jnp.arange(n_uniq // low, dtype=I32)[None, :]).astype(BF16)
        grid_ids = uniq_loc.reshape(n_uniq // low, low)
        near = dot(hot, (grid_ids // 256).astype(BF16)) * 256.0 + dot(hot, (grid_ids % 256).astype(BF16))
        mine = inv_loc[:, None] % low == jnp.arange(low, dtype=I32)[None, :]
        tok_id = jnp.sum(jnp.where(mine, near, 0.0), axis=1).astype(I32)
        order = lax.sort(tok_id * n_tok + iota)
        perm = order % n_tok
        sid = order // n_tok
        is_new = jnp.concatenate([jnp.ones((1,), jnp.bool_), sid[1:] != sid[:-1]])
        rank = jnp.cumsum(is_new.astype(I32)) - 1
        used = lax.sort(jnp.where(is_new, sid, jnp.int32(2 ** 30)))[:n_uniq]
        owners = jnp.arange(group_size, dtype=I32)
        own = sid // shard_rows
        own_hot = own[None, :] == owners[:, None]
        cnt = jnp.sum(jnp.where(own_hot & is_new[None, :], 1, 0), axis=1).astype(I32)
        first = (jnp.cumsum(cnt) - cnt).astype(I32)
        n_ch = (cnt + CH - 1) // CH
        first_ch = (jnp.cumsum(n_ch) - n_ch).astype(I32)
        pos = rank + jnp.sum(jnp.where(own_hot, (first_ch * CH - first)[:, None], 0), axis=0)
        pos = pos.astype(I32)
        wst = pos.reshape(n_tok // SUB, SUB)[:, 0] // CH
        cid = jnp.arange(row_chunks, dtype=I32)[None, :]
        in_own = (cid >= first_ch[:, None]) & (cid < (first_ch + n_ch)[:, None])
        chunk = jnp.sum(jnp.where(in_own, owners[:, None] * cap_ch + cid - first_ch[:, None], 0), axis=0).astype(I32)
        half_ch = cap_ch // 2
        over_ch = jnp.maximum(n_ch - half_ch, 0)
        over_first = (jnp.cumsum(over_ch) - over_ch).astype(I32)
        fits = over_first + over_ch <= half_ch
        k_ch = cid - first_ch[:, None]
        over_dest = jnp.where(fits, group_size * half_ch + over_first - half_ch,
                              (group_size + 1) * half_ch + (owners - 1) * half_ch)
        dest = jnp.where(k_ch < half_ch, owners[:, None] * half_ch + k_ch, over_dest[:, None] + k_ch)
        dest = jnp.sum(jnp.where(in_own, dest, 0), axis=0).astype(I32)
        unfit = jnp.any(~fits).astype(I32)
        total = jnp.sum(n_ch).astype(I32).reshape(1)
        used_pad = jnp.concatenate([used, jnp.full((capacity,), -1, I32)])
        kk = jnp.arange(capacity, dtype=I32)
        send_ids = jnp.stack([
            jnp.where(kk < cnt[j], lax.dynamic_slice(used_pad, (first[j],), (capacity,)), -1)
            for j in range(group_size)])
        notes = jnp.where(jnp.arange(128)[None, :] == 0, over_first[:, None], unfit)
        mail = lax.all_to_all(jnp.concatenate([send_ids, notes], axis=1), 'emb', 0, 0)
        recv_ids = mail[:, :capacity]
        valid = recv_ids >= 0
        local_row = recv_ids - my_dev * shard_rows
        fetch_row = jnp.where(valid, local_row, 0).reshape(-1)
        add_line = line_of(jnp.where(valid, local_row, shard_rows).reshape(-1))
        fetch_line = line_of(fetch_row)
        recv_cnt = jnp.sum(valid.astype(I32), axis=1).astype(I32)
        half = capacity // 2
        n_base = jnp.minimum(recv_cnt, half)
        beyond = jnp.maximum(recv_cnt - half, 0)
        at_over = mail[:, capacity]
        fitted = at_over + (beyond + CH - 1) // CH <= half_ch
        n_over = jnp.where(fitted, beyond, 0)
        at_over = jnp.where(fitted, at_over, 0)
        n_rest = jnp.where(fitted, 0, beyond)
        any_rest = jnp.max(mail[:, capacity + 1])
        posc = pos.reshape(n_tok, 1)
        posr = pos.reshape(n_tok // SUB, 1, SUB)

        tok_spec = pl.BlockSpec((TB, d_model), lambda i, *_: (i, 0))
        posr_spec = pl.BlockSpec((TB // SUB, 1, SUB), lambda i, *_: (i, 0, 0))
        grid = (n_tok // TB,)
        tok_out = jax.ShapeDtypeStruct((n_tok, d_model), BF16)

        def w_specs(layer, *shapes):
            return [once((1,) + s, lambda i, *_, layer=layer: (layer, 0, 0)) for s in shapes]

        s_up, s_dn, s_sq = (d_model, ff), (ff, d_model), (d_model, d_emb)
        mm = 2.0 * n_tok * d_model * ff
        sq = 2.0 * n_tok * d_model * d_emb

        def forward(layer, x, returned):
            return pl.pallas_call(
                fwd_kernel, out_shape=[tok_out] * 3,
                grid_spec=pltpu.PrefetchScalarGridSpec(
                    num_scalar_prefetch=2, grid=grid,
                    in_specs=[tok_spec, pl.BlockSpec((TB, 1), lambda i, *_: (i, 0)),
                              *w_specs(layer, s_up, s_dn, s_sq, s_sq), ANY],
                    out_specs=[tok_spec] * 3,
                    scratch_shapes=[pltpu.VMEM((n_rows, d_emb), BF16), pltpu.SemaphoreType.DMA]),
                compiler_params=params(), name='fwd',
                cost_estimate=cost(2 * mm + 2 * sq, 3e7),
            )(wst, chunk, x, posc, w_up, w_down, w_gate, w_proj, returned)

        send_out = [jax.ShapeDtypeStruct((r, d_emb), F32) for r in (slots // 2, half, slots // 2)]
        row_scratch = [pltpu.VMEM((n_rows, d_emb), F32), pltpu.SemaphoreType.DMA]

        def rowgrad_top(layer, x, c):
            return pl.pallas_call(
                rowgrad_top_kernel, out_shape=[tok_out, *send_out],
                grid_spec=pltpu.PrefetchScalarGridSpec(
                    num_scalar_prefetch=3, grid=grid,
                    in_specs=[tok_spec, tok_spec, posr_spec, *w_specs(layer, s_sq, s_sq)],
                    out_specs=[tok_spec, ANY, ANY, ANY], scratch_shapes=row_scratch),
                compiler_params=params(), name='rowgrad',
                cost_estimate=cost(2 * sq, 3e7),
            )(wst, dest, total, x, c, posr, w_gate, w_proj)

        def backward(layer, x, c, s, e, g_below):
            return pl.pallas_call(
                bwd_kernel, out_shape=[tok_out, tok_out, *send_out],
                grid_spec=pltpu.PrefetchScalarGridSpec(
                    num_scalar_prefetch=3, grid=grid,
                    in_specs=[tok_spec] * 4 + w_specs(layer, s_up, s_dn, s_sq)
                    + [tok_spec, posr_spec] + w_specs(layer - 1, s_sq),
                    out_specs=[tok_spec, tok_spec, ANY, ANY, ANY], scratch_shapes=row_scratch),
                compiler_params=params(), name='bwd',
                cost_estimate=cost(3 * mm + 4 * sq, 6e7),
            )(wst, dest, total, x, c, s, e, w_up, w_down, w_gate, g_below, posr, w_proj)

        half_spec = pl.BlockSpec((half * PIECES, 128), lambda i, *_: (i, 0))
        acc_scratch = [pltpu.VMEM(((shard_rows + 8) * PIECES + PAD, 128), F32),
                       pltpu.VMEM((8 * PIECES + PAD, 128), F32), pltpu.SemaphoreType.DMA]
        lines_out = jax.ShapeDtypeStruct((layers * shard_rows * PIECES, 128), F32)

        def scatter(layer, received, grads):
            return pl.pallas_call(
                functools.partial(scatter_kernel, layer), out_shape=lines_out,
                grid_spec=pltpu.PrefetchScalarGridSpec(
                    num_scalar_prefetch=4, grid=(group_size,),
                    in_specs=[half_spec, half_spec, ANY], out_specs=ANY, scratch_shapes=acc_scratch),
                compiler_params=params(), name='scatter', input_output_aliases={6: 0},
                cost_estimate=cost(1e10, 4e7),
            )(add_line, n_base, n_over, at_over, to_lines(received[0]), to_lines(received[1]), grads)

        def scatter_many(order, received):
            def at_layer(at):
                return pl.BlockSpec(
                    (half * PIECES, 128),
                    lambda p, i, *_: (jnp.where(p == at, i, jnp.where(p < at, 0, group_size - 1)), 0))

            return pl.pallas_call(
                functools.partial(scatter_many_kernel, order), out_shape=lines_out,
                grid_spec=pltpu.PrefetchScalarGridSpec(
                    num_scalar_prefetch=4, grid=(len(order), group_size),
                    in_specs=[at_layer(at) for at in range(len(order)) for _ in range(2)], out_specs=ANY,
                    scratch_shapes=[pltpu.VMEM((2 * (shard_rows + 8) * PIECES + PAD, 128), F32),
                                    pltpu.VMEM((8 * PIECES + PAD, 128), F32), pltpu.SemaphoreType.DMA((2,))]),
                compiler_params=pltpu.CompilerParams(dimension_semantics=('arbitrary', 'arbitrary'),
                                                     vmem_limit_bytes=VMEM_LIMIT),
                name='scatter_many', cost_estimate=cost(4e10, 1.6e8),
            )(add_line, n_base, n_over, at_over, *[to_lines(a) for pair in received for a in pair])

        def scatter_rest(layer, received, grads):
            return pl.pallas_call(
                functools.partial(rest_kernel, layer), out_shape=lines_out,
                grid_spec=pltpu.PrefetchScalarGridSpec(
                    num_scalar_prefetch=2, grid=(group_size,),
                    in_specs=[half_spec, ANY], out_specs=ANY, scratch_shapes=acc_scratch),
                compiler_params=params(), name='scatter_rest', input_output_aliases={3: 0},
                cost_estimate=cost(1e10, 4e7),
            )(add_line, n_rest, to_lines(received), grads)

        def send_home(a):
            return exchange(a.reshape(group_size, half, d_emb)).reshape(slots // 2, d_emb)

        def gather(source, layer, line, src_rows):
            n = source.shape[1]
            steps = n // src_rows
            return pl.pallas_call(
                functools.partial(gather_kernel, steps),
                out_shape=jax.ShapeDtypeStruct((line.shape[0], d_emb), BF16),
                grid_spec=pltpu.PrefetchScalarGridSpec(
                    num_scalar_prefetch=1, grid=(steps + line.shape[0] // TB,),
                    in_specs=[pl.BlockSpec((1, src_rows, d_emb),
                                           lambda i, *_: (layer, jnp.minimum(i, steps - 1), 0))],
                    out_specs=pl.BlockSpec((TB, d_emb), lambda i, *_: (jnp.maximum(i - steps, 0), 0)),
                    scratch_shapes=[pltpu.VMEM((n * PIECES + PAD, 128), F32),
                                    pltpu.VMEM((TB * PIECES + PAD, 128), F32)]),
                compiler_params=params(),
                cost_estimate=cost(1e10, 2e7),
            )(line, source)

        def tok_gather(a, rows):
            return gather(a.reshape(1, n_tok, d_model), 0, line_of(rows), n_tok // 4)

        def serve(layer, line):
            return gather(tab_loc, layer, line, shard_rows // 3).reshape(group_size, capacity, d_emb)

        def exchange(a):
            return lax.all_to_all(a, 'emb', 0, 0)

        served = serve(0, fetch_line)
        got = exchange(served)
        perm, unperm, served, later = lax.optimization_barrier((perm, perm * n_tok + iota, served, fetch_line))
        unperm = lax.sort(unperm) % n_tok
        x = tok_gather(x_loc, perm)
        c = tok_gather(dy_loc, perm)
        ready = [serve(layer, later) for layer in range(1, min(3, layers))]
        saved_x, saved_e, saved_g = [], [], []
        for layer in range(layers):
            here = got
            if layer + 1 < layers:
                x, c, unperm, here, ready, later = lax.optimization_barrier((x, c, unperm, here, ready, later))
                got = exchange(ready.pop(0))
                if layer + 3 < layers:
                    ready.append(serve(layer + 3, later))
            saved_x.append(x)
            x, e, g = forward(layer, x, here.reshape(slots, d_emb))
            saved_e.append(e)
            saved_g.append(g)
        x_out = tok_gather(x, unperm)

        rests = []
        homes = []
        s, base, over, rest = rowgrad_top(layers - 1, saved_x[layers - 1], c)
        for layer in reversed(range(layers)):
            rests.append((layer, rest))
            base = send_home(base)
            homes.append((base, lax.all_gather(over, 'emb', axis=0, tiled=True)))
            if layer > 0:
                if len(homes) > 1:
                    c, homes[-2] = lax.optimization_barrier((c, homes[-2]))
                c, s, base, over, rest = backward(layer, saved_x[layer], c, s, saved_e[layer], saved_g[layer - 1])
        grads = scatter_many(tuple(range(layers - 1, 0, -1)), homes[:-1])
        grads = scatter(0, homes[-1], grads)

        def add_rest(state):
            left, acc = state
            for layer, rest in rests:
                rest, left = lax.optimization_barrier((rest, left))
                acc = scatter_rest(layer, send_home(rest), acc)
            return left - 1, acc

        grads = lax.while_loop(lambda state: state[0] > 0, add_rest, (any_rest, grads))[1]
        return x_out, from_lines(grads, layers * shard_rows, d_emb).reshape(layers, shard_rows, d_emb)

    return jax.shard_map(body, mesh=mesh,
                         in_specs=(P('emb'), P('emb'), P('emb', None), P('emb', None), P(None, 'emb', None),
                                   P(), P(), P(), P()),
                         out_specs=(P('emb', None), P(None, 'emb', None)), check_vma=False)
```
